256 devices in a mesh: grp: 2 (over core), blk: 128 (over y, z, x).
Axes of the slice: x: 4, y: 4, z: 8, core: 2. Of those that a mesh axis runs over, the one named last changes fastest.
Arguments:
- field: bfloat16 [256, 1048576], P('blk', 'grp'), may hold values from -4 to 4
- response: float32 [65], replicated, may hold values from 0.3 to 1
- area_weight: float32 [1048576], P(('grp', 'blk')), may hold values from 0.3 to 3
Outputs:
- patterns: float32 [256, 1048576], P(None, ('grp', 'blk'))
- scaled_r: float32 [256, 256], replicated
The draws below stay inside these ranges and needn't reach their ends.
All inputs are finite; a program needn't handle non-finite values.
Results may differ from the reference program's by a relative error of at most 0.00055.
Values may be sent and summed in bfloat16 or wider, within the bound.
A program may use at most 128 MiB of HBM per device.

```python
import math
import jax
import jax.numpy as jnp
from jax import lax

MONTHS = 128
MEMBERS = 2
COLS = 256
BINS = 65
POINTS = 1048576


def draw_field(key, part):
    subkeys = jax.random.split(key, 5)
    mode_total = 32
    decades = 1.2
    amplitude = 4.0
    smooth_share = 0.6
    noise_level = 0.2
    uncorrelated_noise = jax.random.truncated_normal(subkeys[0], -4.0, 4.0, (COLS, POINTS), jnp.float32) * noise_level
    jagged_share = math.sqrt(1.0 - smooth_share * smooth_share)
    mode_order = jnp.arange(mode_total, dtype=jnp.float32)
    strength = amplitude * jnp.power(10.0, -decades * mode_order / (mode_total - 1))
    temporal = jax.random.normal(subkeys[1], (COLS, mode_total), jnp.float32) * strength[None, :] / math.sqrt(COLS)
    cycles = jax.random.randint(subkeys[2], (mode_total, 1), 1, 9).astype(jnp.float32)
    phases = jax.random.uniform(subkeys[3], (mode_total, 1), jnp.float32, -math.pi, math.pi)
    places = jnp.arange(POINTS, dtype=jnp.float32)[None, :] / POINTS
    smoothed_signal = math.sqrt(2.0) * jnp.cos(2.0 * math.pi * cycles * places + phases)
    jagged = jax.random.truncated_normal(subkeys[4], -4.0, 4.0, (mode_total, POINTS), jnp.float32)
    spatial = smooth_share * smoothed_signal + jagged_share * jagged
    mode_part = jnp.dot(temporal, spatial, precision=lax.Precision.HIGHEST)
    return jnp.clip(mode_part + uncorrelated_noise, -4.0, 4.0).astype(jnp.bfloat16)


def shard_levels(rng, dims, pieces, smallest, largest):
    def one(axis_at, blocks):
        steps = jax.random.uniform(jax.random.fold_in(jax.random.fold_in(rng, 6), axis_at), (blocks,), jnp.float32, smallest / len(pieces), largest / len(pieces))
        return jnp.repeat(jnp.exp(steps), dims[axis_at] // blocks).reshape((-1,) + (1,) * (len(dims) - axis_at - 1))

    level = one(*pieces[0])
    for cut in pieces[1:]:
        level = level * one(*cut)
    return level


def setup_inputs(seed: int = 0) -> dict:
    arg_keys = jax.random.split(jax.random.key(seed), 4)
    return {
        "field": draw_field(jax.random.fold_in(arg_keys[3], 71), 0),
        "response": jnp.clip(jax.random.uniform(arg_keys[1], (BINS,), jnp.float32, 0.3, 1.0), 0.3, 1.0),
        "area_weight": jnp.clip(jnp.exp(math.log(3.0) - 2.3025851 * jax.random.uniform(arg_keys[2], (POINTS,), jnp.float32) ** shard_levels(arg_keys[2], (POINTS,), ((0, 256),), -0.2, 0.2)), 0.3, 3.0),
    }


def reference(field, response, area_weight):
    time_series = field.astype(jnp.float32).reshape(MEMBERS, MONTHS, POINTS)
    spectrum = jnp.fft.rfft(time_series, axis=1) * response[None, :, None]
    lowpass_result = jnp.fft.irfft(spectrum, n=MONTHS, axis=1)
    data = (lowpass_result.reshape(COLS, POINTS) * area_weight[None, :]).T
    q_factor, r_factor = jnp.linalg.qr(data, mode='reduced')
    signs = jnp.sign(jnp.diagonal(r_factor))
    r_factor = r_factor * signs[:, None]
    q_factor = q_factor * signs[None, :]
    scale = jnp.sqrt(jnp.float32(POINTS))
    return (q_factor.T * scale, r_factor / scale)
```

```python
import functools

import jax
import jax.numpy as jnp
import numpy as np
from jax import lax
from jax.experimental import pallas as pl
from jax.experimental.pallas import tpu as pltpu
from jax.sharding import PartitionSpec as P

MONTHS = 128
COLS = 256
ROWS = 4096
TOP = lax.Precision.HIGHEST
NY, NZ, NX = 4, 8, 4
NB = NY * NZ * NX
CHUNK = 512


def solve_lower(matrix, rhs):
    return lax.linalg.triangular_solve(matrix, rhs, left_side=True, lower=True)


def filter_matrix(response):
    months = MONTHS
    bins = response.shape[0]
    freq = np.arange(bins)
    edge = (freq == 0) | (freq == months // 2)
    coef = np.where(edge, 1.0, 2.0) / months
    angle = 2.0 * np.pi * ((np.arange(months)[:, None] * freq[None, :]) % months) / months
    cos = np.cos(angle).astype(np.float32)
    sin = np.sin(angle).astype(np.float32)
    basis = jnp.asarray(np.concatenate([cos, sin], axis=1))
    gain = jnp.asarray(coef.astype(np.float32)) * response
    return jnp.dot(basis * jnp.concatenate([gain, gain])[None, :], basis.T, precision=TOP)


def split3(value):
    high = value.astype(jnp.bfloat16)
    rest = value - high.astype(jnp.float32)
    middle = rest.astype(jnp.bfloat16)
    low = (rest - middle.astype(jnp.float32)).astype(jnp.bfloat16)
    return high, middle, low


def dot_t(a, b):
    return lax.dot_general(a, b, (((1,), (1,)), ((), ())), preferred_element_type=jnp.float32)


def gather_kernel(
    field_ref, weight_ref, f_ref, g_ref,
    fbuf, gacc, pbuf, hbuf, s1buf, s2buf, tbuf,
    own_sem, a_send, a_recv, p_send, p_recv, s1_send, s1_recv, s2_send, s2_recv, s3_send, s3_recv,
):
    core = lax.axis_index("grp")
    me = lax.axis_index("blk")
    my = me // (NZ * NX)
    mz = (me // NX) % NZ
    mx = me % NX
    mxy = my * NX + mx
    other = 1 - core

    def xy_peer(p):
        return (p // NX) * (NZ * NX) + mz * NX + p % NX

    def z_peer(p):
        return my * (NZ * NX) + p * NX + mx

    barrier = pltpu.get_barrier_semaphore()

    def greet(k, _):
        pl.semaphore_signal(barrier, inc=1, device_id={"blk": (me + k) % NB})
        return 0

    lax.fori_loop(1, NB, greet, 0)
    pl.semaphore_signal(barrier, inc=1, device_id={"grp": other})
    pl.semaphore_wait(barrier, NB)

    def cut(p):
        return field_ref.at[:, pl.ds(pl.multiple_of(p * ROWS, ROWS), ROWS)]

    def send_copy(p):
        return pltpu.make_async_remote_copy(
            src_ref=cut(p), dst_ref=fbuf.at[me], send_sem=a_send.at[p], recv_sem=a_recv.at[me],
            device_id={"blk": p})

    def recv_copy(p):
        return pltpu.make_async_remote_copy(
            src_ref=cut(p), dst_ref=fbuf.at[p], send_sem=a_send.at[p], recv_sem=a_recv.at[p],
            device_id={"blk": p})

    def send(k, _):
        send_copy((me + k) % NB).start()
        return 0

    lax.fori_loop(1, NB, send, 0)
    own = pltpu.make_async_copy(cut(me), fbuf.at[me], own_sem)
    own.start()
    gacc[...] = jnp.zeros_like(gacc)
    own.wait()

    def arrive(k, _):
        recv_copy((me + k) % NB).wait_recv()
        return 0

    lax.fori_loop(1, NB, arrive, 0)

    def gram(c, _):
        lanes = pl.ds(pl.multiple_of(c * CHUNK, CHUNK), CHUNK)
        block = fbuf[:, :, lanes].reshape(COLS, CHUNK)
        f_ref[:, lanes] = block
        w = weight_ref[:, lanes]
        weighted = block.astype(jnp.float32) * (w * w)
        high, middle, low = split3(weighted)
        gacc[...] += dot_t(block, low) + dot_t(block, middle) + dot_t(block, high)
        return 0

    lax.fori_loop(0, ROWS // CHUNK, gram, 0)

    half = COLS // 2

    def rows(start, n):
        return pl.ds(pl.multiple_of(start, n), n)

    pair = pltpu.make_async_remote_copy(
        src_ref=gacc.at[rows(other * half, half)], dst_ref=pbuf, send_sem=p_send.at[0], recv_sem=p_recv.at[0],
        device_id={"grp": other})
    pair.start()
    pair.wait()
    hbuf[...] = gacc[rows(core * half, half), :] + pbuf[...]

    def s1(p, slot):
        return pltpu.make_async_remote_copy(
            src_ref=hbuf.at[rows(p * 8, 8)], dst_ref=s1buf.at[slot], send_sem=s1_send.at[p], recv_sem=s1_recv.at[slot],
            device_id={"blk": xy_peer(p)})

    def s2(p, slot):
        return pltpu.make_async_remote_copy(
            src_ref=tbuf.at[0], dst_ref=s2buf.at[slot], send_sem=s2_send.at[p], recv_sem=s2_recv.at[slot],
            device_id={"blk": z_peer(p)})

    def s3(p, slot):
        return pltpu.make_async_remote_copy(
            src_ref=tbuf.at[1], dst_ref=g_ref.at[rows(core * half + slot * 8, 8)],
            send_sem=s3_send.at[p], recv_sem=s3_recv.at[slot], device_id={"blk": xy_peer(p)})

    for k in range(1, 16):
        s1((mxy + k) % 16, mxy).start()
    total = hbuf[rows(mxy * 8, 8), :]
    for k in range(1, 16):
        p = (mxy + k) % 16
        s1(p, p).wait_recv()
        total = total + s1buf[p]
    tbuf[0] = total
    s2buf[mz] = total
    for k in range(1, 8):
        s2((mz + k) % 8, mz).start()
    for k in range(1, 8):
        p = (mz + k) % 8
        s2(p, p).wait_recv()
    total = s2buf[0]
    for k in range(1, 8):
        total = total + s2buf[k]
    tbuf[1] = total
    g_ref[rows(core * half + mxy * 8, 8), :] = total
    for k in range(1, 16):
        s3((mxy + k) % 16, mxy).start()
    for k in range(1, 16):
        p = (mxy + k) % 16
        s3(p, p).wait_recv()
    back = pltpu.make_async_remote_copy(
        src_ref=g_ref.at[rows(core * half, half)], dst_ref=g_ref.at[rows(core * half, half)],
        send_sem=p_send.at[1], recv_sem=p_recv.at[1], device_id={"grp": other})
    back.start()
    back.wait()
    for k in range(1, 16):
        p = (mxy + k) % 16
        s1(p, p).wait_send()
        s3(p, p).wait_send()
    for k in range(1, 8):
        p = (mz + k) % 8
        s2(p, p).wait_send()

    def sent(k, _):
        send_copy((me + k) % NB).wait_send()
        return 0

    lax.fori_loop(1, NB, sent, 0)


def gather_and_gram(field, weight):
    dma = pltpu.SemaphoreType.DMA
    vmem = pl.BlockSpec(memory_space=pltpu.VMEM)
    return pl.pallas_call(
        gather_kernel,
        out_shape=(
            jax.ShapeDtypeStruct((COLS, ROWS), jnp.bfloat16),
            jax.ShapeDtypeStruct((COLS, COLS), jnp.float32),
        ),
        in_specs=[pl.BlockSpec(memory_space=pl.ANY), vmem],
        out_specs=(vmem, vmem),
        scratch_shapes=[
            pltpu.VMEM((NB, 2, ROWS), jnp.bfloat16),
            pltpu.VMEM((COLS, COLS), jnp.float32),
            pltpu.VMEM((COLS // 2, COLS), jnp.float32),
            pltpu.VMEM((COLS // 2, COLS), jnp.float32),
            pltpu.VMEM((16, 8, COLS), jnp.float32),
            pltpu.VMEM((8, 8, COLS), jnp.float32),
            pltpu.VMEM((2, 8, COLS), jnp.float32),
            dma, dma((NB,)), dma((NB,)), dma((2,)), dma((2,)),
            dma((16,)), dma((16,)), dma((8,)), dma((8,)), dma((16,)), dma((16,)),
        ],
        compiler_params=pltpu.CompilerParams(
            collective_id=0, has_side_effects=True, vmem_limit_bytes=40 * 1024 * 1024),
        name="gather_gram",
    )(field, weight)


def shards(field, response, area_weight):
    weight = area_weight.reshape(1, ROWS)
    gathered, raw = gather_and_gram(field, weight)
    total = jnp.float32(ROWS * lax.axis_size("grp") * lax.axis_size("blk"))
    mixing = filter_matrix(response)
    zero = jnp.zeros_like(mixing)
    both = jnp.concatenate(
        [jnp.concatenate([mixing, zero], axis=1), jnp.concatenate([zero, mixing], axis=1)], axis=0)
    gram = jnp.dot(jnp.dot(both, raw / total, precision=TOP), both.T, precision=TOP)
    lower = jnp.linalg.cholesky(gram)
    solver = solve_lower(lower, both)
    patterns = jnp.dot(solver, gathered.astype(jnp.float32), precision=TOP) * weight
    return patterns, lower.T


def solution(mesh):
    in_specs = (P("blk", "grp"), P(), P(("grp", "blk")))
    out_specs = (P(None, ("grp", "blk")), P())
    return jax.shard_map(shards, mesh=mesh, in_specs=in_specs, out_specs=out_specs, check_vma=False)
```

```python
import jax
import jax.numpy as jnp
import numpy as np
from jax import lax
from jax.experimental import pallas as pl
from jax.experimental.pallas import tpu as pltpu
from jax.sharding import PartitionSpec as P

MONTHS = 128
COLS = 256
BINS = MONTHS // 2 + 1
ROWS = 4096
POINTS = 1048576
TOP = lax.Precision.HIGHEST
NY, NZ, NX = 4, 8, 4
NB = NY * NZ * NX
CHUNK = 512
BLOCK = 16
WIDE = 384
OUT_CHUNK = 512


def filter_tables():
    freq = np.arange(BINS)
    edge = (freq == 0) | (freq == MONTHS // 2)
    coef = np.where(edge, 1.0, 2.0) / MONTHS
    angle = 2.0 * np.pi * ((np.arange(MONTHS)[:, None] * freq[None, :]) % MONTHS) / MONTHS
    cos, sin = np.cos(angle), np.sin(angle)
    return np.stack([cos, sin, cos * coef, sin * coef]).astype(np.float32)


def split3(value):
    high = value.astype(jnp.bfloat16)
    rest = value - high.astype(jnp.float32)
    middle = rest.astype(jnp.bfloat16)
    low = (rest - middle.astype(jnp.float32)).astype(jnp.bfloat16)
    return high, middle, low


def dot_t(a, b, precision=None):
    return lax.dot_general(a, b, (((1,), (1,)), ((), ())), precision=precision, preferred_element_type=jnp.float32)


def row_of(tile, s):
    return jnp.broadcast_to(tile[s:s + 1, :], (8, 128))


def eliminate(work):
    sub = lax.broadcasted_iota(jnp.int32, (8, 128), 0)
    for b in range(COLS // BLOCK):
        r0 = b * BLOCK
        base = 0 if r0 < MONTHS else MONTHS
        lane = r0 - base
        top = [work[r0:r0 + 8, base + 128 * t:base + 128 * t + 128] for t in range(3)]
        bot = [work[r0 + 8:r0 + 16, base + 128 * t:base + 128 * t + 128] for t in range(3)]
        ct = [jnp.broadcast_to(top[0][:, lane + j:lane + j + 1], (8, 128)) for j in range(8)]
        cb = [jnp.broadcast_to(bot[0][:, lane + j:lane + j + 1], (8, 128)) for j in range(16)]
        for j in range(BLOCK):
            if j < 8:
                d = lax.rsqrt(row_of(ct[j], j))
                lt = jnp.where(sub > j, ct[j] * d, 0.0)
                lb = cb[j] * d
                for k in range(j + 1, 8):
                    f = row_of(lt, k)
                    ct[k] = ct[k] - lt * f
                    cb[k] = cb[k] - lb * f
                for k in range(8, 16):
                    cb[k] = cb[k] - lb * row_of(lb, k - 8)
                for t in range(3):
                    u = row_of(top[t], j) * d
                    bot[t] = bot[t] - lb * u
                    top[t] = jnp.where(sub == j, u, top[t] - lt * u)
            else:
                i = j - 8
                d = lax.rsqrt(row_of(cb[j], i))
                lb = jnp.where(sub > i, cb[j] * d, 0.0)
                for k in range(j + 1, 16):
                    cb[k] = cb[k] - lb * row_of(lb, k - 8)
                for t in range(3):
                    u = row_of(bot[t], i) * d
                    bot[t] = jnp.where(sub == i, u, bot[t] - lb * u)
        for t in range(3):
            work[r0:r0 + 8, base + 128 * t:base + 128 * t + 128] = top[t]
            work[r0 + 8:r0 + 16, base + 128 * t:base + 128 * t + 128] = bot[t]
        nxt = r0 + BLOCK
        if nxt < COLS:
            panel = jnp.concatenate([jnp.concatenate(top, axis=1), jnp.concatenate(bot, axis=1)], axis=0)
            h, m, l = split3(panel)
            first = nxt // 128 * 128
            left = first - base
            width = COLS - first
            cut = lambda x: x[:, left:left + width]
            a = jnp.concatenate([cut(h), cut(h), cut(m), cut(h), cut(l), cut(m)], axis=0)
            c = jnp.concatenate([h, m, h, l, h, m], axis=0)
            prod = lax.dot_general(a, c, (((0,), (0,)), ((), ())), preferred_element_type=jnp.float32)
            work[nxt:COLS, base:base + WIDE] = work[nxt:COLS, base:base + WIDE] - prod[nxt - first:, :]


def solve_kernel(raw_ref, filt_ref, weight_ref, f_ref, out_ref, r_ref, work, fbuf, obuf, fsem, osem):
    load = pltpu.make_async_copy(f_ref, fbuf, fsem)
    load.start()
    mix = filt_ref[...]
    half = MONTHS
    scaled = raw_ref[...] * (1.0 / POINTS)

    def side(block):
        return jnp.dot(mix, dot_t(block, mix, TOP), precision=TOP, preferred_element_type=jnp.float32)

    zero = jnp.zeros((half, half), jnp.float32)
    work[:half, :half] = side(scaled[:half, :half])
    work[:half, half:2 * half] = side(scaled[:half, half:])
    work[half:, half:2 * half] = side(scaled[half:, half:])
    work[half:, :half] = zero
    work[:half, 2 * half:3 * half] = mix
    work[:half, 3 * half:] = zero
    work[half:, 2 * half:3 * half] = zero
    work[half:, 3 * half:] = mix
    eliminate(work)
    r = lax.broadcasted_iota(jnp.int32, (COLS, COLS), 0)
    c = lax.broadcasted_iota(jnp.int32, (COLS, COLS), 1)
    r_ref[...] = jnp.where(r <= c, work[:, :COLS], 0.0)
    th, tm, tl = split3(work[:, COLS:])
    load.wait()
    n = ROWS // OUT_CHUNK

    def put(i):
        return pltpu.make_async_copy(
            obuf.at[i], out_ref.at[:, pl.ds(pl.multiple_of(i * OUT_CHUNK, OUT_CHUNK), OUT_CHUNK)], osem.at[i])

    def chunk(i, _):
        lanes = pl.ds(pl.multiple_of(i * OUT_CHUNK, OUT_CHUNK), OUT_CHUNK)
        f = fbuf[:, lanes]
        dot = lambda t: jnp.dot(t, f, preferred_element_type=jnp.float32)
        obuf[i] = (dot(tl) + dot(tm) + dot(th)) * weight_ref[:, lanes]
        put(i).start()
        return 0

    lax.fori_loop(0, n, chunk, 0)

    def done(i, _):
        put(i).wait()
        return 0

    lax.fori_loop(0, n, done, 0)


def solve(raw, filt, weight, gathered):
    vmem = pl.BlockSpec(memory_space=pltpu.VMEM)
    hbm = pl.BlockSpec(memory_space=pl.ANY)
    n = ROWS // OUT_CHUNK
    return pl.pallas_call(
        solve_kernel,
        out_shape=(jax.ShapeDtypeStruct((COLS, ROWS), jnp.float32), jax.ShapeDtypeStruct((COLS, COLS), jnp.float32)),
        in_specs=[vmem, vmem, vmem, hbm],
        out_specs=(hbm, vmem),
        scratch_shapes=[
            pltpu.VMEM((COLS, 4 * MONTHS), jnp.float32),
            pltpu.VMEM((COLS, ROWS), jnp.bfloat16),
            pltpu.VMEM((n, COLS, OUT_CHUNK), jnp.float32),
            pltpu.SemaphoreType.DMA, pltpu.SemaphoreType.DMA((n,)),
        ],
        compiler_params=pltpu.CompilerParams(vmem_limit_bytes=60 * 1024 * 1024),
        name="solve",
    )(raw, filt, weight, gathered)


def gather_kernel(
    field_ref, weight_ref, response_ref, table_ref, f_ref, g_ref, filt_ref,
    fbuf, gacc, pbuf, hbuf, s1buf, s2buf, tbuf,
    own_sem, a_send, a_recv, p_send, p_recv, s1_send, s1_recv, s2_send, s2_recv, s3_send, s3_recv,
):
    core = lax.axis_index("grp")
    me = lax.axis_index("blk")
    my = me // (NZ * NX)
    mz = (me // NX) % NZ
    mx = me % NX
    mxy = my * NX + mx
    other = 1 - core

    def xy_peer(p):
        return (p // NX) * (NZ * NX) + mz * NX + p % NX

    def z_peer(p):
        return my * (NZ * NX) + p * NX + mx

    barrier = pltpu.get_barrier_semaphore()

    def greet(k, _):
        pl.semaphore_signal(barrier, inc=1, device_id={"blk": (me + k) % NB})
        return 0

    lax.fori_loop(1, NB, greet, 0)
    pl.semaphore_signal(barrier, inc=1, device_id={"grp": other})
    pl.semaphore_wait(barrier, NB)

    def cut(p):
        return field_ref.at[:, pl.ds(pl.multiple_of(p * ROWS, ROWS), ROWS)]

    def send_copy(p):
        return pltpu.make_async_remote_copy(
            src_ref=cut(p), dst_ref=fbuf.at[me], send_sem=a_send.at[p], recv_sem=a_recv.at[me],
            device_id={"blk": p})

    def recv_copy(p):
        return pltpu.make_async_remote_copy(
            src_ref=cut(p), dst_ref=fbuf.at[p], send_sem=a_send.at[p], recv_sem=a_recv.at[p],
            device_id={"blk": p})

    def send(k, _):
        send_copy((me + k) % NB).start()
        return 0

    lax.fori_loop(1, NB, send, 0)
    own = pltpu.make_async_copy(cut(me), fbuf.at[me], own_sem)
    own.start()
    gacc[...] = jnp.zeros_like(gacc)
    gain = response_ref[...]
    filt_ref[...] = (
        dot_t(table_ref[2] * gain, table_ref[0], TOP) + dot_t(table_ref[3] * gain, table_ref[1], TOP))
    own.wait()

    def arrive(k, _):
        recv_copy((me + k) % NB).wait_recv()
        return 0

    lax.fori_loop(1, NB, arrive, 0)

    def gram(c, _):
        lanes = pl.ds(pl.multiple_of(c * CHUNK, CHUNK), CHUNK)
        block = fbuf[:, :, lanes].reshape(COLS, CHUNK)
        f_ref[:, lanes] = block
        w = weight_ref[:, lanes]
        weighted = block.astype(jnp.float32) * (w * w)
        high, middle, low = split3(weighted)
        gacc[...] += dot_t(block, low) + dot_t(block, middle) + dot_t(block, high)
        return 0

    lax.fori_loop(0, ROWS // CHUNK, gram, 0)

    half = COLS // 2

    def rows(start, n):
        return pl.ds(pl.multiple_of(start, n), n)

    pair = pltpu.make_async_remote_copy(
        src_ref=gacc.at[rows(other * half, half)], dst_ref=pbuf, send_sem=p_send.at[0], recv_sem=p_recv.at[0],
        device_id={"grp": other})
    pair.start()
    pair.wait()
    hbuf[...] = gacc[rows(core * half, half), :] + pbuf[...]

    def s1(p, slot):
        return pltpu.make_async_remote_copy(
            src_ref=hbuf.at[rows(p * 8, 8)], dst_ref=s1buf.at[slot], send_sem=s1_send.at[p], recv_sem=s1_recv.at[slot],
            device_id={"blk": xy_peer(p)})

    def s2(p, slot):
        return pltpu.make_async_remote_copy(
            src_ref=tbuf.at[0], dst_ref=s2buf.at[slot], send_sem=s2_send.at[p], recv_sem=s2_recv.at[slot],
            device_id={"blk": z_peer(p)})

    def s3(p, slot):
        return pltpu.make_async_remote_copy(
            src_ref=tbuf.at[1], dst_ref=g_ref.at[rows(core * half + slot * 8, 8)],
            send_sem=s3_send.at[p], recv_sem=s3_recv.at[slot], device_id={"blk": xy_peer(p)})

    for k in range(1, 16):
        s1((mxy + k) % 16, mxy).start()
    total = hbuf[rows(mxy * 8, 8), :]
    for k in range(1, 16):
        p = (mxy + k) % 16
        s1(p, p).wait_recv()
        total = total + s1buf[p]
    tbuf[0] = total
    s2buf[mz] = total
    for k in range(1, 8):
        s2((mz + k) % 8, mz).start()
    for k in range(1, 8):
        p = (mz + k) % 8
        s2(p, p).wait_recv()
    total = s2buf[0]
    for k in range(1, 8):
        total = total + s2buf[k]
    tbuf[1] = total
    g_ref[rows(core * half + mxy * 8, 8), :] = total
    for k in range(1, 16):
        s3((mxy + k) % 16, mxy).start()
    for k in range(1, 16):
        p = (mxy + k) % 16
        s3(p, p).wait_recv()
    back = pltpu.make_async_remote_copy(
        src_ref=g_ref.at[rows(core * half, half)], dst_ref=g_ref.at[rows(core * half, half)],
        send_sem=p_send.at[1], recv_sem=p_recv.at[1], device_id={"grp": other})
    back.start()
    back.wait()
    for k in range(1, 16):
        p = (mxy + k) % 16
        s1(p, p).wait_send()
        s3(p, p).wait_send()
    for k in range(1, 8):
        p = (mz + k) % 8
        s2(p, p).wait_send()

    def sent(k, _):
        send_copy((me + k) % NB).wait_send()
        return 0

    lax.fori_loop(1, NB, sent, 0)


def gather_and_gram(field, weight, response, table):
    dma = pltpu.SemaphoreType.DMA
    vmem = pl.BlockSpec(memory_space=pltpu.VMEM)
    return pl.pallas_call(
        gather_kernel,
        out_shape=(
            jax.ShapeDtypeStruct((COLS, ROWS), jnp.bfloat16),
            jax.ShapeDtypeStruct((COLS, COLS), jnp.float32),
            jax.ShapeDtypeStruct((MONTHS, MONTHS), jnp.float32),
        ),
        in_specs=[pl.BlockSpec(memory_space=pl.ANY), vmem, vmem, vmem],
        out_specs=(vmem, vmem, vmem),
        scratch_shapes=[
            pltpu.VMEM((NB, 2, ROWS), jnp.bfloat16),
            pltpu.VMEM((COLS, COLS), jnp.float32),
            pltpu.VMEM((COLS // 2, COLS), jnp.float32),
            pltpu.VMEM((COLS // 2, COLS), jnp.float32),
            pltpu.VMEM((16, 8, COLS), jnp.float32),
            pltpu.VMEM((8, 8, COLS), jnp.float32),
            pltpu.VMEM((2, 8, COLS), jnp.float32),
            dma, dma((NB,)), dma((NB,)), dma((2,)), dma((2,)),
            dma((16,)), dma((16,)), dma((8,)), dma((8,)), dma((16,)), dma((16,)),
        ],
        compiler_params=pltpu.CompilerParams(
            collective_id=0, has_side_effects=True, vmem_limit_bytes=60 * 1024 * 1024),
        name="gather_gram",
    )(field, weight, response, table)


def shards(field, response, area_weight):
    weight = area_weight.reshape(1, ROWS)
    gathered, raw, filt = gather_and_gram(field, weight, response.reshape(1, BINS), jnp.asarray(filter_tables()))
    return solve(raw, filt, weight, gathered)


def solution(mesh):
    in_specs = (P("blk", "grp"), P(), P(("grp", "blk")))
    out_specs = (P(None, ("grp", "blk")), P())
    return jax.shard_map(shards, mesh=mesh, in_specs=in_specs, out_specs=out_specs, check_vma=False)
```

```python
import jax
import jax.numpy as jnp
import numpy as np
from jax import lax
from jax.experimental import pallas as pl
from jax.experimental.pallas import tpu as pltpu
from jax.sharding import PartitionSpec as P

MONTHS = 128
COLS = 256
BINS = MONTHS // 2 + 1
ROWS = 4096
POINTS = 1048576
TOP = lax.Precision.HIGHEST
NY, NZ, NX = 4, 8, 4
NB = NY * NZ * NX
PLANE = NZ * NX
GROUP = 2 * PLANE
CHUNK = 1024
BLOCK = 16
WIDE = 384
OUT_CHUNK = 512
OUT_STEPS = ROWS // OUT_CHUNK


def filter_tables():
    freq = np.arange(BINS)
    edge = (freq == 0) | (freq == MONTHS // 2)
    coef = np.where(edge, 1.0, 2.0) / MONTHS
    angle = 2.0 * np.pi * ((np.arange(MONTHS)[:, None] * freq[None, :]) % MONTHS) / MONTHS
    cos, sin = np.cos(angle), np.sin(angle)
    return np.stack([cos, sin, cos * coef, sin * coef]).astype(np.float32)


def split3(value):
    high = value.astype(jnp.bfloat16)
    rest = value - high.astype(jnp.float32)
    middle = rest.astype(jnp.bfloat16)
    low = (rest - middle.astype(jnp.float32)).astype(jnp.bfloat16)
    return high, middle, low


def dot_t(a, b, precision=None):
    return lax.dot_general(a, b, (((1,), (1,)), ((), ())), precision=precision, preferred_element_type=jnp.float32)


def aligned(start, n):
    return pl.ds(pl.multiple_of(start, n), n)


def row_of(tile, s):
    return jnp.broadcast_to(tile[s:s + 1, :], (8, 128))


def eliminate(work, b):
    sub = lax.broadcasted_iota(jnp.int32, (8, 128), 0)
    r0 = b * BLOCK
    base = 0 if r0 < MONTHS else MONTHS
    lane = r0 - base
    top = [work[r0:r0 + 8, base + 128 * t:base + 128 * t + 128] for t in range(3)]
    bot = [work[r0 + 8:r0 + 16, base + 128 * t:base + 128 * t + 128] for t in range(3)]
    ct = [jnp.broadcast_to(top[0][:, lane + j:lane + j + 1], (8, 128)) for j in range(8)]
    cb = [jnp.broadcast_to(bot[0][:, lane + j:lane + j + 1], (8, 128)) for j in range(16)]
    for j in range(BLOCK):
        if j < 8:
            d = lax.rsqrt(row_of(ct[j], j))
            lt = jnp.where(sub > j, ct[j] * d, 0.0)
            lb = cb[j] * d
            for k in range(j + 1, 8):
                f = row_of(lt, k)
                ct[k] = ct[k] - lt * f
                cb[k] = cb[k] - lb * f
            for k in range(8, 16):
                cb[k] = cb[k] - lb * row_of(lb, k - 8)
            for t in range(3):
                u = row_of(top[t], j) * d
                bot[t] = bot[t] - lb * u
                top[t] = jnp.where(sub == j, u, top[t] - lt * u)
        else:
            i = j - 8
            d = lax.rsqrt(row_of(cb[j], i))
            lb = jnp.where(sub > i, cb[j] * d, 0.0)
            for k in range(j + 1, 16):
                cb[k] = cb[k] - lb * row_of(lb, k - 8)
            for t in range(3):
                u = row_of(bot[t], i) * d
                bot[t] = jnp.where(sub == i, u, bot[t] - lb * u)
    for t in range(3):
        work[r0:r0 + 8, base + 128 * t:base + 128 * t + 128] = top[t]
        work[r0 + 8:r0 + 16, base + 128 * t:base + 128 * t + 128] = bot[t]
    nxt = r0 + BLOCK
    if nxt == COLS:
        return
    panel = jnp.concatenate([jnp.concatenate(top, axis=1), jnp.concatenate(bot, axis=1)], axis=0)
    h, m, l = split3(panel)
    first = nxt // 128 * 128
    left = first - base
    width = COLS - first
    cut = lambda x: x[:, left:left + width]
    a = jnp.concatenate([cut(h), cut(h), cut(m), cut(h), cut(l), cut(m)], axis=0)
    c = jnp.concatenate([h, m, h, l, h, m], axis=0)
    prod = lax.dot_general(a, c, (((0,), (0,)), ((), ())), preferred_element_type=jnp.float32)
    work[nxt:COLS, base:base + WIDE] = work[nxt:COLS, base:base + WIDE] - prod[nxt - first:, :]


def solve_kernel(raw_ref, filt_ref, weight_ref, f_ref, out_ref, r_ref, work, obuf, osem):
    mix = filt_ref[...]
    half = MONTHS

    def side(block):
        return jnp.dot(mix, dot_t(block, mix, TOP), precision=TOP, preferred_element_type=jnp.float32)

    def fold(i, j):
        first = raw_ref[i * half:(i + 1) * half, j * half:(j + 1) * half]
        second = raw_ref[j * half:(j + 1) * half, i * half:(i + 1) * half]
        return (first + second.T) * (1.0 / POINTS)

    zero = jnp.zeros((half, half), jnp.float32)
    work[:half, :half] = side(fold(0, 0))
    work[:half, half:2 * half] = side(fold(0, 1))
    work[half:, half:2 * half] = side(fold(1, 1))
    work[half:, :half] = zero
    work[:half, 2 * half:3 * half] = mix
    work[:half, 3 * half:] = zero
    work[half:, 2 * half:3 * half] = zero
    work[half:, 3 * half:] = mix

    def put(i, k):
        return pltpu.make_async_copy(
            obuf.at[i, aligned(k * half, half)],
            out_ref.at[aligned(k * half, half), aligned(i * OUT_CHUNK, OUT_CHUNK)], osem.at[k, i])

    def project(i, k, terms, depth):
        lanes = aligned(i * OUT_CHUNK, OUT_CHUNK)
        f = f_ref[:depth, lanes]
        dot = lambda t: jnp.dot(t, f, preferred_element_type=jnp.float32)
        high, middle, low = terms
        obuf[i, k * half:(k + 1) * half, :] = (dot(low) + dot(middle) + dot(high)) * weight_ref[:, lanes]
        put(i, k).start()

    for b in range(8):
        eliminate(work, b)
    upper = split3(work[:half, 2 * half:3 * half])
    for b in range(8, 16):
        eliminate(work, b)
        project(b - 8, 0, upper, half)
    lower = split3(work[half:, 2 * half:])

    def step(i, _):
        project(i, 1, lower, COLS)
        return 0

    lax.fori_loop(0, OUT_STEPS, step, 0)
    r = lax.broadcasted_iota(jnp.int32, (COLS, COLS), 0)
    c = lax.broadcasted_iota(jnp.int32, (COLS, COLS), 1)
    r_ref[...] = jnp.where(r <= c, work[:, :COLS], 0.0)

    def done(i, _):
        put(i, 0).wait()
        put(i, 1).wait()
        return 0

    lax.fori_loop(0, OUT_STEPS, done, 0)


def solve(raw, filt, weight, gathered):
    vmem = pl.BlockSpec(memory_space=pltpu.VMEM)
    hbm = pl.BlockSpec(memory_space=pltpu.HBM)
    return pl.pallas_call(
        solve_kernel,
        out_shape=(jax.ShapeDtypeStruct((COLS, ROWS), jnp.float32), jax.ShapeDtypeStruct((COLS, COLS), jnp.float32)),
        in_specs=[vmem, vmem, vmem, vmem],
        out_specs=(hbm, vmem),
        scratch_shapes=[
            pltpu.VMEM((COLS, 4 * MONTHS), jnp.float32),
            pltpu.VMEM((OUT_STEPS, COLS, OUT_CHUNK), jnp.float32),
            pltpu.SemaphoreType.DMA((2, OUT_STEPS)),
        ],
        compiler_params=pltpu.CompilerParams(vmem_limit_bytes=16 * 1024 * 1024),
        name="solve",
    )(raw, filt, weight, gathered)


def gather_kernel(
    field_ref, weight_in, response_in, table_in, f_ref, g_ref, filt_ref, weight_ref,
    response_ref, table_ref, fbuf, gacc, terms, pbuf, hbuf, s1buf, s2buf, tbuf,
    phase, own_sem, a_send, a_recv, p_send, p_recv, s1_send, s1_recv, s2_send, s2_recv, s3_send, s3_recv,
):
    core = lax.axis_index("grp")
    me = lax.axis_index("blk")
    my = me // PLANE
    mz = (me // NX) % NZ
    mx = me % NX
    mxy = my * NX + mx
    other = 1 - core

    def at(y, z, x):
        return (y % NY) * PLANE + (z % NZ) * NX + x % NX

    def xy_peer(p):
        return at(p // NX, mz, p % NX)

    def signal(sem, **where):
        pl.semaphore_signal(sem, inc=1, device_id=where)

    def cut(p):
        return field_ref.at[:, aligned(p * ROWS, ROWS)]

    def copy(p, slot):
        return pltpu.make_async_remote_copy(
            src_ref=cut(p), dst_ref=fbuf.at[slot], send_sem=a_send.at[p], recv_sem=a_recv.at[slot],
            device_id={"blk": p})

    barrier = pltpu.get_barrier_semaphore()
    for k in range(1, NZ):
        signal(barrier, blk=at(my, mz + k, mx))
    for k in range(1, NX):
        signal(barrier, blk=at(my, mz, mx + k))
    for k in range(1, NY):
        signal(barrier, blk=at(my + k, mz, mx))
    signal(barrier, grp=other)
    pl.semaphore_wait(barrier, NZ + NX + NY - 2)
    for k in range(1, NX):
        signal(phase.at[0], blk=at(my, mz, mx + k))

    def send_line(i, _):
        copy(at(my, mz + i, mx), me).start()
        return 0

    lax.fori_loop(1, NZ, send_line, 0)
    local = [
        pltpu.make_async_copy(cut(me), fbuf.at[me], own_sem.at[0]),
        pltpu.make_async_copy(weight_in, weight_ref, own_sem.at[1]),
        pltpu.make_async_copy(response_in, response_ref, own_sem.at[2]),
        pltpu.make_async_copy(table_in, table_ref, own_sem.at[3]),
    ]
    for each in local:
        each.start()
    pl.semaphore_wait(phase.at[0], NX - 1)
    for k in range(1, NY):
        signal(phase.at[1], blk=at(my + k, mz, mx))

    def send_plane(i, _):
        copy(at(my, mz + i % NZ, mx + 1 + i // NZ), me).start()
        return 0

    lax.fori_loop(0, PLANE - NZ, send_plane, 0)
    pl.semaphore_wait(phase.at[1], NY - 1)

    def send_rest(i, _):
        copy(at(my + 1 + i // PLANE, mz + i % NZ, mx + (i // NZ) % NX), me).start()
        return 0

    lax.fori_loop(0, NB - PLANE, send_rest, 0)

    f_ref[...] = jnp.zeros_like(f_ref)
    for each in local:
        each.wait()
    gain = response_ref[...]
    filt_ref[...] = (
        dot_t(table_ref[2] * gain, table_ref[0], TOP) + dot_t(table_ref[3] * gain, table_ref[1], TOP))

    def window(t, _):
        group = (my + NY - t) % NY

        def arrive(i, _):
            p = group * PLANE + (mz * NX + mx + i) % PLANE
            copy(p, p).wait_recv()
            return 0

        lax.fori_loop(jnp.where(t == 0, 1, 0), PLANE, arrive, 0)
        rows = aligned(group * GROUP, GROUP)
        terms[...] = jnp.zeros_like(terms)

        def gram(c, _):
            lanes = aligned(c * CHUNK, CHUNK)
            block = fbuf[aligned(group * PLANE, PLANE), :, lanes].reshape(GROUP, CHUNK)
            f_ref[rows, lanes] = block
            w = weight_ref[:, lanes]
            pieces = jnp.concatenate(split3(block.astype(jnp.float32) * (w * w)), axis=0)
            terms[...] += dot_t(pieces, f_ref[:, lanes])
            return 0

        lax.fori_loop(0, ROWS // CHUNK, gram, 0)
        total = terms[2 * GROUP:, :] + terms[GROUP:2 * GROUP, :] + terms[:GROUP, :]
        column = lax.broadcasted_iota(jnp.int32, (GROUP, COLS), 1)
        gacc[rows, :] = jnp.where(column // GROUP == group, 0.5 * total, total)
        return 0

    lax.fori_loop(0, NY, window, 0)

    half = COLS // 2
    pair = pltpu.make_async_remote_copy(
        src_ref=gacc.at[aligned(other * half, half)], dst_ref=pbuf, send_sem=p_send, recv_sem=p_recv,
        device_id={"grp": other})
    pair.start()
    pair.wait()
    hbuf[...] = gacc[aligned(core * half, half), :] + pbuf[...]

    def s1(p, slot):
        return pltpu.make_async_remote_copy(
            src_ref=hbuf.at[aligned(p * 8, 8)], dst_ref=s1buf.at[slot], send_sem=s1_send.at[p], recv_sem=s1_recv.at[slot],
            device_id={"blk": xy_peer(p)})

    def s2(p, slot):
        return pltpu.make_async_remote_copy(
            src_ref=tbuf.at[0], dst_ref=s2buf.at[slot], send_sem=s2_send.at[p], recv_sem=s2_recv.at[slot],
            device_id={"blk": at(my, p, mx)})

    def s3(p, c, slot):
        return pltpu.make_async_remote_copy(
            src_ref=tbuf.at[1], dst_ref=g_ref.at[aligned(slot * 8, 8)],
            send_sem=s3_send.at[c * 16 + p], recv_sem=s3_recv.at[slot], device_id={"blk": xy_peer(p), "grp": c})

    xy = [(mxy + k) % 16 for k in range(1, 16)]
    line = [(mz + k) % NZ for k in range(1, NZ)]
    for p in xy:
        s1(p, mxy).start()
    total = hbuf[aligned(mxy * 8, 8), :]
    for p in xy:
        s1(p, p).wait_recv()
        total = total + s1buf[p]
    tbuf[0] = total
    s2buf[mz] = total
    for p in line:
        s2(p, mz).start()
    for p in line:
        s2(p, p).wait_recv()
    total = s2buf[0]
    for k in range(1, NZ):
        total = total + s2buf[k]
    tbuf[1] = total
    mine = core * 16 + mxy
    g_ref[aligned(mine * 8, 8), :] = total
    for p in xy:
        s3(p, core, mine).start()
        s3(p, other, mine).start()
    s3(mxy, other, mine).start()
    for p in xy:
        s3(p, core, core * 16 + p).wait_recv()
        s3(p, other, other * 16 + p).wait_recv()
    s3(mxy, other, other * 16 + mxy).wait_recv()
    for p in xy:
        s1(p, p).wait_send()
        s3(p, core, mine).wait_send()
        s3(p, other, mine).wait_send()
    s3(mxy, other, mine).wait_send()
    for p in line:
        s2(p, p).wait_send()

    def sent(k, _):
        copy((me + k) % NB, me).wait_send()
        return 0

    lax.fori_loop(1, NB, sent, 0)


def gather_and_gram(field, weight, response, table):
    dma = pltpu.SemaphoreType.DMA
    vmem = pl.BlockSpec(memory_space=pltpu.VMEM)
    hbm = pl.BlockSpec(memory_space=pltpu.HBM)
    return pl.pallas_call(
        gather_kernel,
        out_shape=(
            jax.ShapeDtypeStruct((COLS, ROWS), jnp.bfloat16),
            jax.ShapeDtypeStruct((COLS, COLS), jnp.float32),
            jax.ShapeDtypeStruct((MONTHS, MONTHS), jnp.float32),
            jax.ShapeDtypeStruct((1, ROWS), jnp.float32),
        ),
        in_specs=[hbm, hbm, hbm, hbm],
        out_specs=(vmem, vmem, vmem, vmem),
        scratch_shapes=[
            pltpu.VMEM((1, BINS), jnp.float32),
            pltpu.VMEM((4, MONTHS, BINS), jnp.float32),
            pltpu.VMEM((NB, 2, ROWS), jnp.bfloat16),
            pltpu.VMEM((COLS, COLS), jnp.float32),
            pltpu.VMEM((3 * GROUP, COLS), jnp.float32),
            pltpu.VMEM((COLS // 2, COLS), jnp.float32),
            pltpu.VMEM((COLS // 2, COLS), jnp.float32),
            pltpu.VMEM((16, 8, COLS), jnp.float32),
            pltpu.VMEM((NZ, 8, COLS), jnp.float32),
            pltpu.VMEM((2, 8, COLS), jnp.float32),
            pltpu.SemaphoreType.REGULAR((2,)),
            dma((4,)), dma((NB,)), dma((NB,)), dma, dma,
            dma((16,)), dma((16,)), dma((NZ,)), dma((NZ,)), dma((32,)), dma((32,)),
        ],
        compiler_params=pltpu.CompilerParams(
            collective_id=0, has_side_effects=True, vmem_limit_bytes=16 * 1024 * 1024),
        name="gather_gram",
    )(field, weight, response, table)


def shards(field, response, area_weight):
    gathered, raw, filt, weight = gather_and_gram(
        *(pltpu.with_memory_space_constraint(x, pltpu.HBM) for x in (field, area_weight.reshape(1, ROWS), response.reshape(1, BINS), jnp.asarray(filter_tables()))))
    return solve(raw, filt, weight, gathered)


def solution(mesh):
    in_specs = (P("blk", "grp"), P(), P(("grp", "blk")))
    out_specs = (P(None, ("grp", "blk")), P())
    return jax.shard_map(shards, mesh=mesh, in_specs=in_specs, out_specs=out_specs, check_vma=False)
```

```python
import jax
import jax.numpy as jnp
import numpy as np
from jax import lax
from jax.experimental import pallas as pl
from jax.experimental.pallas import tpu as pltpu
from jax.sharding import PartitionSpec as P

MONTHS = 128
COLS = 256
BINS = MONTHS // 2 + 1
ROWS = 4096
POINTS = 1048576
TOP = lax.Precision.HIGHEST
NY, NZ, NX = 4, 8, 4
NB = NY * NZ * NX
PLANE = NZ * NX
GROUP = 2 * PLANE
CHUNK = 1024
BLOCK = 16
WIDE = 384
OUT_CHUNK = 512
OUT_STEPS = ROWS // OUT_CHUNK


def filter_tables():
    freq = np.arange(BINS)
    edge = (freq == 0) | (freq == MONTHS // 2)
    coef = np.where(edge, 1.0, 2.0) / MONTHS
    angle = 2.0 * np.pi * ((np.arange(MONTHS)[:, None] * freq[None, :]) % MONTHS) / MONTHS
    cos, sin = np.cos(angle), np.sin(angle)
    return np.stack([cos, sin, cos * coef, sin * coef]).astype(np.float32)


def split3(value):
    high = value.astype(jnp.bfloat16)
    rest = value - high.astype(jnp.float32)
    middle = rest.astype(jnp.bfloat16)
    low = (rest - middle.astype(jnp.float32)).astype(jnp.bfloat16)
    return high, middle, low


def dot_t(a, b, precision=None):
    return lax.dot_general(a, b, (((1,), (1,)), ((), ())), precision=precision, preferred_element_type=jnp.float32)


def aligned(start, n):
    return pl.ds(pl.multiple_of(start, n), n)


def row_of(tile, s):
    return jnp.broadcast_to(tile[s:s + 1, :], (8, 128))


def eliminate(work, b):
    sub = lax.broadcasted_iota(jnp.int32, (8, 128), 0)
    r0 = b * BLOCK
    base = 0 if r0 < MONTHS else MONTHS
    lane = r0 - base
    top = [work[r0:r0 + 8, base + 128 * t:base + 128 * t + 128] for t in range(3)]
    bot = [work[r0 + 8:r0 + 16, base + 128 * t:base + 128 * t + 128] for t in range(3)]
    ct = [jnp.broadcast_to(top[0][:, lane + j:lane + j + 1], (8, 128)) for j in range(8)]
    cb = [jnp.broadcast_to(bot[0][:, lane + j:lane + j + 1], (8, 128)) for j in range(16)]
    for j in range(BLOCK):
        if j < 8:
            d = lax.rsqrt(row_of(ct[j], j))
            lt = jnp.where(sub > j, ct[j] * d, 0.0)
            lb = cb[j] * d
            for k in range(j + 1, 8):
                f = row_of(lt, k)
                ct[k] = ct[k] - lt * f
                cb[k] = cb[k] - lb * f
            for k in range(8, 16):
                cb[k] = cb[k] - lb * row_of(lb, k - 8)
            for t in range(3):
                u = row_of(top[t], j) * d
                bot[t] = bot[t] - lb * u
                top[t] = jnp.where(sub == j, u, top[t] - lt * u)
        else:
            i = j - 8
            d = lax.rsqrt(row_of(cb[j], i))
            lb = jnp.where(sub > i, cb[j] * d, 0.0)
            for k in range(j + 1, 16):
                cb[k] = cb[k] - lb * row_of(lb, k - 8)
            for t in range(3):
                u = row_of(bot[t], i) * d
                bot[t] = jnp.where(sub == i, u, bot[t] - lb * u)
    for t in range(3):
        work[r0:r0 + 8, base + 128 * t:base + 128 * t + 128] = top[t]
        work[r0 + 8:r0 + 16, base + 128 * t:base + 128 * t + 128] = bot[t]
    nxt = r0 + BLOCK
    if nxt == COLS:
        return
    panel = jnp.concatenate([jnp.concatenate(top, axis=1), jnp.concatenate(bot, axis=1)], axis=0)
    h, m, l = split3(panel)
    first = nxt // 128 * 128
    left = first - base
    width = COLS - first
    cut = lambda x: x[:, left:left + width]
    a = jnp.concatenate([cut(h), cut(h), cut(m), cut(h), cut(l), cut(m)], axis=0)
    c = jnp.concatenate([h, m, h, l, h, m], axis=0)
    prod = lax.dot_general(a, c, (((0,), (0,)), ((), ())), preferred_element_type=jnp.float32)
    work[nxt:COLS, base:base + WIDE] = work[nxt:COLS, base:base + WIDE] - prod[nxt - first:, :]


def solve_kernel(raw_ref, filt_ref, weight_ref, f_ref, out_ref, r_ref, work, obuf, osem):
    mix = filt_ref[...]
    half = MONTHS

    def side(block):
        return jnp.dot(mix, dot_t(block, mix, TOP), precision=TOP, preferred_element_type=jnp.float32)

    def fold(i, j):
        first = raw_ref[i * half:(i + 1) * half, j * half:(j + 1) * half]
        second = raw_ref[j * half:(j + 1) * half, i * half:(i + 1) * half]
        return (first + second.T) * (1.0 / POINTS)

    zero = jnp.zeros((half, half), jnp.float32)
    work[:half, :half] = side(fold(0, 0))
    work[:half, half:2 * half] = side(fold(0, 1))
    work[half:, half:2 * half] = side(fold(1, 1))
    work[half:, :half] = zero
    work[:half, 2 * half:3 * half] = mix
    work[:half, 3 * half:] = zero
    work[half:, 2 * half:3 * half] = zero
    work[half:, 3 * half:] = mix

    def put(i, first, count):
        return pltpu.make_async_copy(
            obuf.at[i, pl.ds(first, count)], out_ref.at[pl.ds(first, count), pl.ds(i * OUT_CHUNK, OUT_CHUNK)],
            osem.at[first // 64, i])

    def stacked(first, count, depth):
        return jnp.concatenate(split3(work[first:first + count, 2 * half:2 * half + depth]), axis=0)

    def project(i, terms, first, count, depth):
        lanes = pl.ds(i * OUT_CHUNK, OUT_CHUNK)
        parts = jnp.dot(terms, f_ref[:depth, lanes], preferred_element_type=jnp.float32)
        total = parts[2 * count:] + parts[count:2 * count] + parts[:count]
        obuf[i, first:first + count, :] = total * weight_ref[:, lanes]
        put(i, first, count).start()

    for b in range(8):
        eliminate(work, b)
    terms = stacked(0, half, half)
    for b in range(8, 12):
        eliminate(work, b)
        for i in (2 * b - 16, 2 * b - 15):
            project(i, terms, 0, half, half)
    terms = stacked(half, 64, COLS)
    for b in range(12, 16):
        eliminate(work, b)
        for i in (2 * b - 24, 2 * b - 23):
            project(i, terms, half, 64, COLS)
    terms = stacked(half + 64, 64, COLS)
    for i in range(OUT_STEPS):
        project(i, terms, half + 64, 64, COLS)
    r = lax.broadcasted_iota(jnp.int32, (COLS, COLS), 0)
    c = lax.broadcasted_iota(jnp.int32, (COLS, COLS), 1)
    r_ref[...] = jnp.where(r <= c, work[:, :COLS], 0.0)

    for i in range(OUT_STEPS):
        put(i, 0, half).wait()
        put(i, half, 64).wait()
        put(i, half + 64, 64).wait()


def solve(raw, filt, weight, gathered):
    vmem = pl.BlockSpec(memory_space=pltpu.VMEM)
    hbm = pl.BlockSpec(memory_space=pltpu.HBM)
    return pl.pallas_call(
        solve_kernel,
        out_shape=(jax.ShapeDtypeStruct((COLS, ROWS), jnp.float32), jax.ShapeDtypeStruct((COLS, COLS), jnp.float32)),
        in_specs=[vmem, vmem, vmem, vmem],
        out_specs=(hbm, vmem),
        scratch_shapes=[
            pltpu.VMEM((COLS, 4 * MONTHS), jnp.float32),
            pltpu.VMEM((OUT_STEPS, COLS, OUT_CHUNK), jnp.float32),
            pltpu.SemaphoreType.DMA((4, OUT_STEPS)),
        ],
        compiler_params=pltpu.CompilerParams(vmem_limit_bytes=16 * 1024 * 1024),
        name="solve",
    )(raw, filt, weight, gathered)


def gather_kernel(
    field_ref, weight_in, response_in, table_in, f_ref, g_ref, filt_ref, weight_ref,
    response_ref, table_ref, fbuf, gacc, terms, pbuf, hbuf, s1buf, s2buf, tbuf,
    phase, own_sem, a_send, a_recv, p_send, p_recv, s1_send, s1_recv, s2_send, s2_recv, s3_send, s3_recv,
):
    core = lax.axis_index("grp")
    me = lax.axis_index("blk")
    my = me // PLANE
    mz = (me // NX) % NZ
    mx = me % NX
    mxy = my * NX + mx
    other = 1 - core

    def at(y, z, x):
        return (y % NY) * PLANE + (z % NZ) * NX + x % NX

    def xy_peer(p):
        return at(p // NX, mz, p % NX)

    def signal(sem, **where):
        pl.semaphore_signal(sem, inc=1, device_id=where)

    def cut(p):
        return field_ref.at[:, aligned(p * ROWS, ROWS)]

    def copy(p, slot):
        return pltpu.make_async_remote_copy(
            src_ref=cut(p), dst_ref=fbuf.at[slot], send_sem=a_send.at[p], recv_sem=a_recv.at[slot],
            device_id={"blk": p})

    barrier = pltpu.get_barrier_semaphore()
    for k in range(1, NZ):
        signal(barrier, blk=at(my, mz + k, mx))
    for k in range(1, NX):
        signal(barrier, blk=at(my, mz, mx + k))
    for k in range(1, NY):
        signal(barrier, blk=at(my + k, mz, mx))
    signal(barrier, grp=other)
    pl.semaphore_wait(barrier, NZ + NX + NY - 2)
    for k in range(1, NX):
        signal(phase.at[0], blk=at(my, mz, mx + k))

    def send_line(i, _):
        copy(at(my, mz + i, mx), me).start()
        return 0

    lax.fori_loop(1, NZ, send_line, 0)
    local = [
        pltpu.make_async_copy(cut(me), fbuf.at[me], own_sem.at[0]),
        pltpu.make_async_copy(weight_in, weight_ref, own_sem.at[1]),
        pltpu.make_async_copy(response_in, response_ref, own_sem.at[2]),
        pltpu.make_async_copy(table_in, table_ref, own_sem.at[3]),
    ]
    for each in local:
        each.start()
    pl.semaphore_wait(phase.at[0], NX - 1)
    for k in range(1, NY):
        signal(phase.at[1], blk=at(my + k, mz, mx))

    def send_plane(i, _):
        copy(at(my, mz + i % NZ, mx + 1 + i // NZ), me).start()
        return 0

    lax.fori_loop(0, PLANE - NZ, send_plane, 0)
    pl.semaphore_wait(phase.at[1], NY - 1)

    def send_rest(i, _):
        copy(at(my + 1 + i // PLANE, mz + i % NZ, mx + (i // NZ) % NX), me).start()
        return 0

    lax.fori_loop(0, NB - PLANE, send_rest, 0)

    f_ref[...] = jnp.zeros_like(f_ref)
    for each in local:
        each.wait()
    gain = response_ref[...]
    filt_ref[...] = (
        dot_t(table_ref[2] * gain, table_ref[0], TOP) + dot_t(table_ref[3] * gain, table_ref[1], TOP))

    share = GROUP // 2
    owner_group = (my + 1) % NY

    def pair(t, group):
        return pltpu.make_async_remote_copy(
            src_ref=gacc.at[aligned(group * GROUP + other * share, share)], dst_ref=pbuf.at[t],
            send_sem=p_send.at[t], recv_sem=p_recv.at[t], device_id={"grp": other})

    def s1(t, i, group, slot):
        return pltpu.make_async_remote_copy(
            src_ref=hbuf.at[t, aligned(i * 8, 8)], dst_ref=s1buf.at[slot], send_sem=s1_send.at[t * NX + i],
            recv_sem=s1_recv.at[slot], device_id={"blk": at(group + NY - 1, mz, i)})

    def s1_from(p):
        return pltpu.make_async_remote_copy(
            src_ref=hbuf.at[0, aligned(0, 8)], dst_ref=s1buf.at[p], send_sem=s1_send.at[0],
            recv_sem=s1_recv.at[p], device_id={"blk": xy_peer(p)})

    def window(t):
        group = (my + NY - t) % NY

        def arrive(i, _):
            p = group * PLANE + (mz * NX + mx + i) % PLANE
            copy(p, p).wait_recv()
            return 0

        lax.fori_loop(jnp.where(t == 0, 1, 0), PLANE, arrive, 0)
        rows = aligned(group * GROUP, GROUP)
        terms[...] = jnp.zeros_like(terms)

        def gram(c, _):
            lanes = aligned(c * CHUNK, CHUNK)
            block = fbuf[aligned(group * PLANE, PLANE), :, lanes].reshape(GROUP, CHUNK)
            f_ref[rows, lanes] = block
            w = weight_ref[:, lanes]
            pieces = jnp.concatenate(split3(block.astype(jnp.float32) * (w * w)), axis=0)
            terms[...] += dot_t(pieces, f_ref[:, lanes])
            return 0

        lax.fori_loop(0, ROWS // CHUNK, gram, 0)
        total = terms[2 * GROUP:, :] + terms[GROUP:2 * GROUP, :] + terms[:GROUP, :]
        column = lax.broadcasted_iota(jnp.int32, (GROUP, COLS), 1)
        gacc[rows, :] = jnp.where(column // GROUP == group, 0.5 * total, total)
        pair(t, group).start()
        pair(t, group).wait_recv()
        hbuf[t] = gacc[aligned(group * GROUP + core * share, share), :] + pbuf[t]
        return group

    def early(t, _):
        group = window(t)
        for i in range(NX):
            s1(t, i, group, mxy).start()
        return 0

    lax.fori_loop(0, NY - 1, early, 0)
    window(NY - 1)
    row = [(mx + k) % NX for k in range(1, NX)]
    for i in row:
        s1(NY - 1, i, owner_group, mxy).start()

    def s2(p, slot):
        return pltpu.make_async_remote_copy(
            src_ref=tbuf.at[0], dst_ref=s2buf.at[slot], send_sem=s2_send.at[p], recv_sem=s2_recv.at[slot],
            device_id={"blk": at(my, p, mx)})

    def piece(p, c):
        y, x = p // NX, p % NX
        return aligned(((y + 1) % NY) * GROUP + c * share + x * 8, 8)

    def s3(p, c, q, d):
        return pltpu.make_async_remote_copy(
            src_ref=tbuf.at[1], dst_ref=g_ref.at[piece(q, d)],
            send_sem=s3_send.at[c * 16 + p], recv_sem=s3_recv.at[d * 16 + q], device_id={"blk": xy_peer(p), "grp": c})

    xy = [(mxy + k) % 16 for k in range(1, 16)]
    line = [(mz + k) % NZ for k in range(1, NZ)]
    total = hbuf[NY - 1, aligned(mx * 8, 8), :]
    for k in range(1, NY):
        for j in range(NX):
            p = (my + k) % NY * NX + j
            s1_from(p).wait_recv()
            total = total + s1buf[p]
    for i in row:
        p = my * NX + i
        s1_from(p).wait_recv()
        total = total + s1buf[p]
    tbuf[0] = total
    s2buf[mz] = total
    for p in line:
        s2(p, mz).start()
    for p in line:
        s2(p, p).wait_recv()
    total = s2buf[0]
    for k in range(1, NZ):
        total = total + s2buf[k]
    tbuf[1] = total
    g_ref[piece(mxy, core), :] = total
    for p in xy:
        s3(p, core, mxy, core).start()
        s3(p, other, mxy, core).start()
    s3(mxy, other, mxy, core).start()
    for p in xy:
        s3(p, core, p, core).wait_recv()
        s3(p, other, p, other).wait_recv()
    s3(mxy, other, mxy, other).wait_recv()
    for p in xy:
        s3(p, core, mxy, core).wait_send()
        s3(p, other, mxy, core).wait_send()
    s3(mxy, other, mxy, core).wait_send()
    for p in line:
        s2(p, p).wait_send()

    def shared(t, _):
        group = (my + NY - t) % NY
        pair(t, group).wait_send()
        for i in range(NX):
            s1(t, i, group, mxy).wait_send()
        return 0

    lax.fori_loop(0, NY - 1, shared, 0)
    pair(NY - 1, owner_group).wait_send()
    for i in row:
        s1(NY - 1, i, owner_group, mxy).wait_send()

    def sent(k, _):
        copy((me + k) % NB, me).wait_send()
        return 0

    lax.fori_loop(1, NB, sent, 0)


def gather_and_gram(field, weight, response, table):
    dma = pltpu.SemaphoreType.DMA
    vmem = pl.BlockSpec(memory_space=pltpu.VMEM)
    hbm = pl.BlockSpec(memory_space=pltpu.HBM)
    return pl.pallas_call(
        gather_kernel,
        out_shape=(
            jax.ShapeDtypeStruct((COLS, ROWS), jnp.bfloat16),
            jax.ShapeDtypeStruct((COLS, COLS), jnp.float32),
            jax.ShapeDtypeStruct((MONTHS, MONTHS), jnp.float32),
            jax.ShapeDtypeStruct((1, ROWS), jnp.float32),
        ),
        in_specs=[hbm, hbm, hbm, hbm],
        out_specs=(vmem, vmem, vmem, vmem),
        scratch_shapes=[
            pltpu.VMEM((1, BINS), jnp.float32),
            pltpu.VMEM((4, MONTHS, BINS), jnp.float32),
            pltpu.VMEM((NB, 2, ROWS), jnp.bfloat16),
            pltpu.VMEM((COLS, COLS), jnp.float32),
            pltpu.VMEM((3 * GROUP, COLS), jnp.float32),
            pltpu.VMEM((NY, GROUP // 2, COLS), jnp.float32),
            pltpu.VMEM((NY, GROUP // 2, COLS), jnp.float32),
            pltpu.VMEM((16, 8, COLS), jnp.float32),
            pltpu.VMEM((NZ, 8, COLS), jnp.float32),
            pltpu.VMEM((2, 8, COLS), jnp.float32),
            pltpu.SemaphoreType.REGULAR((2,)),
            dma((4,)), dma((NB,)), dma((NB,)), dma((NY,)), dma((NY,)),
            dma((16,)), dma((16,)), dma((NZ,)), dma((NZ,)), dma((32,)), dma((32,)),
        ],
        compiler_params=pltpu.CompilerParams(
            collective_id=0, has_side_effects=True, vmem_limit_bytes=16 * 1024 * 1024),
        name="gather_gram",
    )(field, weight, response, table)


def shards(field, response, area_weight):
    gathered, raw, filt, weight = gather_and_gram(
        *(pltpu.with_memory_space_constraint(x, pltpu.HBM) for x in (field, area_weight.reshape(1, ROWS), response.reshape(1, BINS), jnp.asarray(filter_tables()))))
    return solve(raw, filt, weight, gathered)


def solution(mesh):
    in_specs = (P("blk", "grp"), P(), P(("grp", "blk")))
    out_specs = (P(None, ("grp", "blk")), P())
    return jax.shard_map(shards, mesh=mesh, in_specs=in_specs, out_specs=out_specs, check_vma=False)
```

```python
import jax
import jax.numpy as jnp
import numpy as np
from jax import lax
from jax.experimental import pallas as pl
from jax.experimental.pallas import tpu as pltpu
from jax.sharding import PartitionSpec as P

MONTHS = 128
COLS = 256
BINS = MONTHS // 2 + 1
ROWS = 4096
POINTS = 1048576
TOP = lax.Precision.HIGHEST
NY, NZ, NX = 4, 8, 4
NB = NY * NZ * NX
PLANE = NZ * NX
GROUP = 2 * PLANE
CHUNK = 1024
BLOCK = 16
WIDE = 384
OUT_CHUNK = 512
OUT_STEPS = ROWS // OUT_CHUNK


def filter_tables():
    freq = np.arange(BINS)
    edge = (freq == 0) | (freq == MONTHS // 2)
    coef = np.where(edge, 1.0, 2.0) / MONTHS
    angle = 2.0 * np.pi * ((np.arange(MONTHS)[:, None] * freq[None, :]) % MONTHS) / MONTHS
    cos, sin = np.cos(angle), np.sin(angle)
    order = np.arange(MONTHS).reshape(-1, NZ, NX, 2).transpose(0, 2, 1, 3).reshape(-1)
    return np.stack([cos[order], sin[order], cos * coef, sin * coef]).astype(np.float32)


def split3(value):
    high = value.astype(jnp.bfloat16)
    rest = value - high.astype(jnp.float32)
    middle = rest.astype(jnp.bfloat16)
    low = (rest - middle.astype(jnp.float32)).astype(jnp.bfloat16)
    return high, middle, low


def dot_t(a, b, precision=None):
    return lax.dot_general(a, b, (((1,), (1,)), ((), ())), precision=precision, preferred_element_type=jnp.float32)


def aligned(start, n):
    return pl.ds(pl.multiple_of(start, n), n)


def row_of(tile, s):
    return jnp.broadcast_to(tile[s:s + 1, :], (8, 128))


def eliminate(work, b):
    sub = lax.broadcasted_iota(jnp.int32, (8, 128), 0)
    r0 = b * BLOCK
    base = 0 if r0 < MONTHS else MONTHS
    lane = r0 - base
    top = [work[r0:r0 + 8, base + 128 * t:base + 128 * t + 128] for t in range(3)]
    bot = [work[r0 + 8:r0 + 16, base + 128 * t:base + 128 * t + 128] for t in range(3)]
    ct = [jnp.broadcast_to(top[0][:, lane + j:lane + j + 1], (8, 128)) for j in range(8)]
    cb = [jnp.broadcast_to(bot[0][:, lane + j:lane + j + 1], (8, 128)) for j in range(16)]
    for j in range(BLOCK):
        if j < 8:
            d = lax.rsqrt(row_of(ct[j], j))
            lt = jnp.where(sub > j, ct[j] * d, 0.0)
            lb = cb[j] * d
            for k in range(j + 1, 8):
                f = row_of(lt, k)
                ct[k] = ct[k] - lt * f
                cb[k] = cb[k] - lb * f
            for k in range(8, 16):
                cb[k] = cb[k] - lb * row_of(lb, k - 8)
            for t in range(3):
                u = row_of(top[t], j) * d
                bot[t] = bot[t] - lb * u
                top[t] = jnp.where(sub == j, u, top[t] - lt * u)
        else:
            i = j - 8
            d = lax.rsqrt(row_of(cb[j], i))
            lb = jnp.where(sub > i, cb[j] * d, 0.0)
            for k in range(j + 1, 16):
                cb[k] = cb[k] - lb * row_of(lb, k - 8)
            for t in range(3):
                u = row_of(bot[t], i) * d
                bot[t] = jnp.where(sub == i, u, bot[t] - lb * u)
    for t in range(3):
        work[r0:r0 + 8, base + 128 * t:base + 128 * t + 128] = top[t]
        work[r0 + 8:r0 + 16, base + 128 * t:base + 128 * t + 128] = bot[t]
    nxt = r0 + BLOCK
    if nxt == COLS:
        return
    panel = jnp.concatenate([jnp.concatenate(top, axis=1), jnp.concatenate(bot, axis=1)], axis=0)
    h, m, l = split3(panel)
    first = nxt // 128 * 128
    left = first - base
    width = COLS - first
    cut = lambda x: x[:, left:left + width]
    a = jnp.concatenate([cut(h), cut(h), cut(m), cut(h), cut(l), cut(m)], axis=0)
    c = jnp.concatenate([h, m, h, l, h, m], axis=0)
    prod = lax.dot_general(a, c, (((0,), (0,)), ((), ())), preferred_element_type=jnp.float32)
    work[nxt:COLS, base:base + WIDE] = work[nxt:COLS, base:base + WIDE] - prod[nxt - first:, :]


def solve_kernel(raw_ref, filt_ref, weight_ref, f_ref, out_ref, r_ref, work, obuf, osem):
    mix = filt_ref[...]
    half = MONTHS

    def side(block):
        return jnp.dot(mix, dot_t(block, mix, TOP), precision=TOP, preferred_element_type=jnp.float32)

    def fold(i, j):
        first = raw_ref[i * half:(i + 1) * half, j * half:(j + 1) * half]
        second = raw_ref[j * half:(j + 1) * half, i * half:(i + 1) * half]
        return (first + second.T) * (1.0 / POINTS)

    zero = jnp.zeros((half, half), jnp.float32)
    work[:half, :half] = side(fold(0, 0))
    work[:half, half:2 * half] = side(fold(0, 1))
    work[half:, half:2 * half] = side(fold(1, 1))
    work[half:, :half] = zero
    work[:half, 2 * half:3 * half] = mix
    work[:half, 3 * half:] = zero
    work[half:, 2 * half:3 * half] = zero
    work[half:, 3 * half:] = mix

    def put(i, first, count):
        return pltpu.make_async_copy(
            obuf.at[i, pl.ds(first, count)], out_ref.at[pl.ds(first, count), pl.ds(i * OUT_CHUNK, OUT_CHUNK)],
            osem.at[first // 64, i])

    def stacked(first, count, depth):
        return jnp.concatenate(split3(work[first:first + count, 2 * half:2 * half + depth]), axis=0)

    def project(i, terms, first, count, depth):
        lanes = pl.ds(i * OUT_CHUNK, OUT_CHUNK)
        parts = jnp.dot(terms, f_ref[:depth, lanes], preferred_element_type=jnp.float32)
        total = parts[2 * count:] + parts[count:2 * count] + parts[:count]
        obuf[i, first:first + count, :] = total * weight_ref[:, lanes]
        put(i, first, count).start()

    for b in range(8):
        eliminate(work, b)
    terms = stacked(0, half, half)
    for b in range(8, 12):
        eliminate(work, b)
        for i in (2 * b - 16, 2 * b - 15):
            project(i, terms, 0, half, half)
    terms = stacked(half, 64, COLS)
    for b in range(12, 16):
        eliminate(work, b)
        for i in (2 * b - 24, 2 * b - 23):
            project(i, terms, half, 64, COLS)
    terms = stacked(half + 64, 64, COLS)
    for i in range(OUT_STEPS):
        project(i, terms, half + 64, 64, COLS)
    r = lax.broadcasted_iota(jnp.int32, (COLS, COLS), 0)
    c = lax.broadcasted_iota(jnp.int32, (COLS, COLS), 1)
    r_ref[...] = jnp.where(r <= c, work[:, :COLS], 0.0)

    for i in range(OUT_STEPS):
        put(i, 0, half).wait()
        put(i, half, 64).wait()
        put(i, half + 64, 64).wait()


def solve(raw, filt, weight, gathered):
    vmem = pl.BlockSpec(memory_space=pltpu.VMEM)
    hbm = pl.BlockSpec(memory_space=pltpu.HBM)
    return pl.pallas_call(
        solve_kernel,
        out_shape=(jax.ShapeDtypeStruct((COLS, ROWS), jnp.float32), jax.ShapeDtypeStruct((COLS, COLS), jnp.float32)),
        in_specs=[vmem, vmem, vmem, vmem],
        out_specs=(hbm, vmem),
        scratch_shapes=[
            pltpu.VMEM((COLS, 4 * MONTHS), jnp.float32),
            pltpu.VMEM((OUT_STEPS, COLS, OUT_CHUNK), jnp.float32),
            pltpu.SemaphoreType.DMA((4, OUT_STEPS)),
        ],
        compiler_params=pltpu.CompilerParams(vmem_limit_bytes=16 * 1024 * 1024),
        name="solve",
    )(raw, filt, weight, gathered)


def gather_kernel(
    field_ref, weight_in, response_in, table_in, f_ref, g_ref, filt_ref, weight_ref,
    response_ref, table_ref, fbuf, gacc, pieces, pbuf, hbuf, s1buf, s2buf, tbuf,
    phase, own_sem, a_send, a_recv, p_send, p_recv, s1_send, s1_recv, s2_send, s2_recv, s3_send, s3_recv,
):
    core = lax.axis_index("grp")
    me = lax.axis_index("blk")
    my = me // PLANE
    mz = (me // NX) % NZ
    mx = me % NX
    mxy = my * NX + mx
    other = 1 - core

    def at(y, z, x):
        return (y % NY) * PLANE + (z % NZ) * NX + x % NX

    def xy_peer(p):
        return at(p // NX, mz, p % NX)

    def signal(sem, **where):
        pl.semaphore_signal(sem, inc=1, device_id=where)

    def slot_of(p):
        return p // PLANE * PLANE + p % NX * NZ + p // NX % NZ

    def cut(p):
        return field_ref.at[:, aligned(p * ROWS, ROWS)]

    def copy(p, source):
        slot = slot_of(source)
        return pltpu.make_async_remote_copy(
            src_ref=cut(p), dst_ref=fbuf.at[slot], send_sem=a_send.at[p], recv_sem=a_recv.at[slot],
            device_id={"blk": p})

    barrier = pltpu.get_barrier_semaphore()
    for k in range(1, NZ):
        signal(barrier, blk=at(my, mz + k, mx))
    for k in range(1, NX):
        signal(barrier, blk=at(my, mz, mx + k))
    for k in range(1, NY):
        signal(barrier, blk=at(my + k, mz, mx))
    signal(barrier, grp=other)
    pl.semaphore_wait(barrier, NZ + NX + NY - 2)
    for k in range(1, NX):
        signal(phase.at[0], blk=at(my, mz, mx + k))

    def send_line(i, _):
        copy(at(my, mz + i, mx), me).start()
        return 0

    lax.fori_loop(1, NZ, send_line, 0)
    local = [
        pltpu.make_async_copy(cut(me), fbuf.at[slot_of(me)], own_sem.at[0]),
        pltpu.make_async_copy(weight_in, weight_ref, own_sem.at[1]),
        pltpu.make_async_copy(response_in, response_ref, own_sem.at[2]),
        pltpu.make_async_copy(table_in, table_ref, own_sem.at[3]),
    ]
    for each in local:
        each.start()
    pl.semaphore_wait(phase.at[0], NX - 1)
    for k in range(1, NY):
        signal(phase.at[1], blk=at(my + k, mz, mx))

    def send_plane(i, _):
        copy(at(my, mz + i % NZ, mx + 1 + i // NZ), me).start()
        return 0

    lax.fori_loop(0, PLANE - NZ, send_plane, 0)
    pl.semaphore_wait(phase.at[1], NY - 1)

    def send_rest(i, _):
        copy(at(my + 1 + i // PLANE, mz + i % NZ, mx + (i // NZ) % NX), me).start()
        return 0

    lax.fori_loop(0, NB - PLANE, send_rest, 0)

    f_ref[...] = jnp.zeros_like(f_ref)
    for each in local:
        each.wait()
    gain = response_ref[...]
    filt_ref[...] = (
        dot_t(table_ref[2] * gain, table_ref[0], TOP) + dot_t(table_ref[3] * gain, table_ref[1], TOP))

    share = GROUP // 2
    owner_group = (my + 1) % NY

    def pair(t, group):
        return pltpu.make_async_remote_copy(
            src_ref=gacc.at[aligned(group * GROUP + other * share, share)], dst_ref=pbuf.at[t],
            send_sem=p_send.at[t], recv_sem=p_recv.at[t], device_id={"grp": other})

    def s1(t, i, group, slot):
        return pltpu.make_async_remote_copy(
            src_ref=hbuf.at[t, aligned(i * 8, 8)], dst_ref=s1buf.at[slot], send_sem=s1_send.at[t * NX + i],
            recv_sem=s1_recv.at[slot], device_id={"blk": at(group + NY - 1, mz, i)})

    def s1_from(p):
        return pltpu.make_async_remote_copy(
            src_ref=hbuf.at[0, aligned(0, 8)], dst_ref=s1buf.at[p], send_sem=s1_send.at[0],
            recv_sem=s1_recv.at[p], device_id={"blk": xy_peer(p)})

    def window(t):
        group = (my + NY - t) % NY

        def batch(q, _):
            x = (mx + NX - q) % NX

            def arrive(i, _):
                p = at(group, mz + i, x)
                copy(p, p).wait_recv()
                return 0

            lax.fori_loop(jnp.where(t + q == 0, 1, 0), NZ, arrive, 0)
            start = x * BLOCK

            def unpack(c, _):
                lanes = aligned(c * CHUNK, CHUNK)
                block = fbuf[aligned(group * PLANE + x * NZ, NZ), :, lanes].reshape(BLOCK, CHUNK)
                f_ref[aligned(group * GROUP + start, BLOCK), lanes] = block
                w = weight_ref[:, lanes]
                for k, part in enumerate(split3(block.astype(jnp.float32) * (w * w))):
                    pieces[aligned(k * GROUP + start, BLOCK), lanes] = part
                return 0

            lax.fori_loop(0, ROWS // CHUNK, unpack, 0)
            return 0

        lax.fori_loop(0, NX, batch, 0)
        rows = aligned(group * GROUP, GROUP)
        terms = dot_t(pieces[...], f_ref[...])
        total = terms[2 * GROUP:, :] + terms[GROUP:2 * GROUP, :] + terms[:GROUP, :]
        column = lax.broadcasted_iota(jnp.int32, (GROUP, COLS), 1)
        gacc[rows, :] = jnp.where(column // GROUP == group, 0.5 * total, total)
        pair(t, group).start()
        pair(t, group).wait_recv()
        hbuf[t] = gacc[aligned(group * GROUP + core * share, share), :] + pbuf[t]
        return group

    def early(t, _):
        group = window(t)
        for i in range(NX):
            s1(t, i, group, mxy).start()
        return 0

    lax.fori_loop(0, NY - 1, early, 0)
    window(NY - 1)
    row = [(mx + k) % NX for k in range(1, NX)]
    for i in row:
        s1(NY - 1, i, owner_group, mxy).start()

    def s2(p, slot):
        return pltpu.make_async_remote_copy(
            src_ref=tbuf.at[0], dst_ref=s2buf.at[slot], send_sem=s2_send.at[p], recv_sem=s2_recv.at[slot],
            device_id={"blk": at(my, p, mx)})

    def piece(p, c):
        y, x = p // NX, p % NX
        return aligned(((y + 1) % NY) * GROUP + c * share + x * 8, 8)

    def s3(p, c, q, d):
        return pltpu.make_async_remote_copy(
            src_ref=tbuf.at[1], dst_ref=g_ref.at[piece(q, d)],
            send_sem=s3_send.at[c * 16 + p], recv_sem=s3_recv.at[d * 16 + q], device_id={"blk": xy_peer(p), "grp": c})

    xy = [(mxy + k) % 16 for k in range(1, 16)]
    line = [(mz + k) % NZ for k in range(1, NZ)]
    total = hbuf[NY - 1, aligned(mx * 8, 8), :]
    for k in range(1, NY):
        for j in range(NX):
            p = (my + k) % NY * NX + j
            s1_from(p).wait_recv()
            total = total + s1buf[p]
    for i in row:
        p = my * NX + i
        s1_from(p).wait_recv()
        total = total + s1buf[p]
    tbuf[0] = total
    s2buf[mz] = total
    for p in line:
        s2(p, mz).start()
    for p in line:
        s2(p, p).wait_recv()
    total = s2buf[0]
    for k in range(1, NZ):
        total = total + s2buf[k]
    tbuf[1] = total
    g_ref[piece(mxy, core), :] = total
    for p in xy:
        s3(p, core, mxy, core).start()
        s3(p, other, mxy, core).start()
    s3(mxy, other, mxy, core).start()
    for p in xy:
        s3(p, core, p, core).wait_recv()
        s3(p, other, p, other).wait_recv()
    s3(mxy, other, mxy, other).wait_recv()
    for p in xy:
        s3(p, core, mxy, core).wait_send()
        s3(p, other, mxy, core).wait_send()
    s3(mxy, other, mxy, core).wait_send()
    for p in line:
        s2(p, p).wait_send()

    def shared(t, _):
        group = (my + NY - t) % NY
        pair(t, group).wait_send()
        for i in range(NX):
            s1(t, i, group, mxy).wait_send()
        return 0

    lax.fori_loop(0, NY - 1, shared, 0)
    pair(NY - 1, owner_group).wait_send()
    for i in row:
        s1(NY - 1, i, owner_group, mxy).wait_send()

    def sent(k, _):
        copy((me + k) % NB, me).wait_send()
        return 0

    lax.fori_loop(1, NB, sent, 0)


def gather_and_gram(field, weight, response, table):
    dma = pltpu.SemaphoreType.DMA
    vmem = pl.BlockSpec(memory_space=pltpu.VMEM)
    hbm = pl.BlockSpec(memory_space=pltpu.HBM)
    return pl.pallas_call(
        gather_kernel,
        out_shape=(
            jax.ShapeDtypeStruct((COLS, ROWS), jnp.bfloat16),
            jax.ShapeDtypeStruct((COLS, COLS), jnp.float32),
            jax.ShapeDtypeStruct((MONTHS, MONTHS), jnp.float32),
            jax.ShapeDtypeStruct((1, ROWS), jnp.float32),
        ),
        in_specs=[hbm, hbm, hbm, hbm],
        out_specs=(vmem, vmem, vmem, vmem),
        scratch_shapes=[
            pltpu.VMEM((1, BINS), jnp.float32),
            pltpu.VMEM((4, MONTHS, BINS), jnp.float32),
            pltpu.VMEM((NB, 2, ROWS), jnp.bfloat16),
            pltpu.VMEM((COLS, COLS), jnp.float32),
            pltpu.VMEM((3 * GROUP, ROWS), jnp.bfloat16),
            pltpu.VMEM((NY, GROUP // 2, COLS), jnp.float32),
            pltpu.VMEM((NY, GROUP // 2, COLS), jnp.float32),
            pltpu.VMEM((16, 8, COLS), jnp.float32),
            pltpu.VMEM((NZ, 8, COLS), jnp.float32),
            pltpu.VMEM((2, 8, COLS), jnp.float32),
            pltpu.SemaphoreType.REGULAR((2,)),
            dma((4,)), dma((NB,)), dma((NB,)), dma((NY,)), dma((NY,)),
            dma((16,)), dma((16,)), dma((NZ,)), dma((NZ,)), dma((32,)), dma((32,)),
        ],
        compiler_params=pltpu.CompilerParams(
            collective_id=0, has_side_effects=True, vmem_limit_bytes=16 * 1024 * 1024),
        name="gather_gram",
    )(field, weight, response, table)


def shards(field, response, area_weight):
    gathered, raw, filt, weight = gather_and_gram(
        *(pltpu.with_memory_space_constraint(x, pltpu.HBM) for x in (field, area_weight.reshape(1, ROWS), response.reshape(1, BINS), jnp.asarray(filter_tables()))))
    return solve(raw, filt, weight, gathered)


def solution(mesh):
    in_specs = (P("blk", "grp"), P(), P(("grp", "blk")))
    out_specs = (P(None, ("grp", "blk")), P())
    return jax.shard_map(shards, mesh=mesh, in_specs=in_specs, out_specs=out_specs, check_vma=False)
```

```python
import jax
import jax.numpy as jnp
import numpy as np
from jax import lax
from jax.experimental import pallas as pl
from jax.experimental.pallas import tpu as pltpu
from jax.sharding import PartitionSpec as P

MONTHS = 128
COLS = 256
BINS = MONTHS // 2 + 1
ROWS = 4096
POINTS = 1048576
TOP = lax.Precision.HIGHEST
NY, NZ, NX = 4, 8, 4
NB = NY * NZ * NX
PLANE = NZ * NX
GROUP = 2 * PLANE
CHUNK = 1024
BLOCK = 16
WIDE = 384
OUT_CHUNK = 512
OUT_STEPS = ROWS // OUT_CHUNK
FAR_FIRST = sorted(((y, x) for y in range(NY) for x in range(NX) if y or x), key=lambda s: -min(s[0], NY - s[0]) - min(s[1], NX - s[1]))


def filter_tables():
    freq = np.arange(BINS)
    edge = (freq == 0) | (freq == MONTHS // 2)
    coef = np.where(edge, 1.0, 2.0) / MONTHS
    angle = 2.0 * np.pi * ((np.arange(MONTHS)[:, None] * freq[None, :]) % MONTHS) / MONTHS
    cos, sin = np.cos(angle), np.sin(angle)
    order = np.arange(MONTHS).reshape(-1, NZ, NX, 2).transpose(0, 2, 1, 3).reshape(-1)
    return np.stack([cos[order], sin[order], cos * coef, sin * coef]).astype(np.float32)


def split3(value):
    high = value.astype(jnp.bfloat16)
    rest = value - high.astype(jnp.float32)
    middle = rest.astype(jnp.bfloat16)
    low = (rest - middle.astype(jnp.float32)).astype(jnp.bfloat16)
    return high, middle, low


def dot_t(a, b, precision=None):
    return lax.dot_general(a, b, (((1,), (1,)), ((), ())), precision=precision, preferred_element_type=jnp.float32)


def aligned(start, n):
    return pl.ds(pl.multiple_of(start, n), n)


def row_of(tile, s):
    return jnp.broadcast_to(tile[s:s + 1, :], (8, 128))


def eliminate(work, b):
    sub = lax.broadcasted_iota(jnp.int32, (8, 128), 0)
    r0 = b * BLOCK
    base = 0 if r0 < MONTHS else MONTHS
    lane = r0 - base
    top = [work[r0:r0 + 8, base + 128 * t:base + 128 * t + 128] for t in range(3)]
    bot = [work[r0 + 8:r0 + 16, base + 128 * t:base + 128 * t + 128] for t in range(3)]
    ct = [jnp.broadcast_to(top[0][:, lane + j:lane + j + 1], (8, 128)) for j in range(8)]
    cb = [jnp.broadcast_to(bot[0][:, lane + j:lane + j + 1], (8, 128)) for j in range(16)]
    for j in range(BLOCK):
        if j < 8:
            d = lax.rsqrt(row_of(ct[j], j))
            lt = ct[j] * d
            lb = cb[j] * d
            for k in range(j + 1, 8):
                f = row_of(ct[j], k) * d if k == j + 1 else row_of(lt, k)
                ct[k] = ct[k] - lt * f
                cb[k] = cb[k] - lb * f
            for k in range(8, 16):
                cb[k] = cb[k] - lb * row_of(lb, k - 8)
            lt = jnp.where(sub > j, lt, 0.0)
            for t in range(3):
                u = row_of(top[t], j) * d
                bot[t] = bot[t] - lb * u
                top[t] = jnp.where(sub == j, u, top[t] - lt * u)
        else:
            i = j - 8
            d = lax.rsqrt(row_of(cb[j], i))
            lb = cb[j] * d
            for k in range(j + 1, 16):
                cb[k] = cb[k] - lb * (row_of(cb[j], k - 8) * d if k == j + 1 else row_of(lb, k - 8))
            lb = jnp.where(sub > i, lb, 0.0)
            for t in range(3):
                u = row_of(bot[t], i) * d
                bot[t] = jnp.where(sub == i, u, bot[t] - lb * u)
    for t in range(3):
        work[r0:r0 + 8, base + 128 * t:base + 128 * t + 128] = top[t]
        work[r0 + 8:r0 + 16, base + 128 * t:base + 128 * t + 128] = bot[t]
    nxt = r0 + BLOCK
    if nxt == COLS:
        return
    panel = jnp.concatenate([jnp.concatenate(top, axis=1), jnp.concatenate(bot, axis=1)], axis=0)
    h, m, l = split3(panel)
    first = nxt // 128 * 128
    left = first - base
    width = COLS - first
    cut = lambda x: x[:, left:left + width]
    a = jnp.concatenate([cut(h), cut(h), cut(m), cut(h), cut(l), cut(m)], axis=0)
    c = jnp.concatenate([h, m, h, l, h, m], axis=0)
    a = a.T
    skip = nxt - first
    for start, stop in ((nxt, nxt + BLOCK), (nxt + BLOCK, COLS)):
        if start < stop:
            prod = jnp.dot(a[start - first:stop - first], c, preferred_element_type=jnp.float32)
            work[start:stop, base:base + WIDE] = work[start:stop, base:base + WIDE] - prod


def solve_kernel(raw_ref, filt_ref, weight_ref, f_ref, out_ref, r_ref, work, obuf, osem):
    mix = filt_ref[...]
    half = MONTHS

    def fold(i, j):
        first = raw_ref[i * half:(i + 1) * half, j * half:(j + 1) * half]
        second = raw_ref[j * half:(j + 1) * half, i * half:(i + 1) * half]
        return (first + second.T) * (1.0 / POINTS)

    zero = jnp.zeros((half, half), jnp.float32)
    sides = [dot_t(fold(0, 0), mix, TOP), dot_t(fold(0, 1), mix, TOP)]
    for rows in (slice(0, BLOCK), slice(BLOCK, half)):
        for k, right in enumerate(sides):
            work[rows, k * half:(k + 1) * half] = jnp.dot(
                mix[rows], right, precision=TOP, preferred_element_type=jnp.float32)
    last = dot_t(fold(1, 1), mix, TOP)
    work[half:, half:2 * half] = jnp.dot(mix, last, precision=TOP, preferred_element_type=jnp.float32)
    work[half:, :half] = zero
    work[:half, 2 * half:3 * half] = mix
    work[:half, 3 * half:] = zero
    work[half:, 2 * half:3 * half] = zero
    work[half:, 3 * half:] = mix

    def put(i, first, count):
        return pltpu.make_async_copy(
            obuf.at[i, pl.ds(first, count)], out_ref.at[pl.ds(first, count), pl.ds(i * OUT_CHUNK, OUT_CHUNK)],
            osem.at[first // 64, i])

    def stacked(first, count, depth):
        return jnp.concatenate(split3(work[first:first + count, 2 * half:2 * half + depth]), axis=0)

    def project(i, terms, first, count, depth):
        lanes = pl.ds(i * OUT_CHUNK, OUT_CHUNK)
        parts = jnp.dot(terms, f_ref[:depth, lanes], preferred_element_type=jnp.float32)
        total = parts[2 * count:] + parts[count:2 * count] + parts[:count]
        obuf[i, first:first + count, :] = total * weight_ref[:, lanes]
        put(i, first, count).start()

    for b in range(8):
        eliminate(work, b)
    terms = stacked(0, half, half)
    for b in range(8, 12):
        eliminate(work, b)
        for i in (2 * b - 16, 2 * b - 15):
            project(i, terms, 0, half, half)
    terms = stacked(half, 64, COLS)
    for b in range(12, 16):
        eliminate(work, b)
        for i in (2 * b - 24, 2 * b - 23):
            project(i, terms, half, 64, COLS)
    terms = stacked(half + 64, 64, COLS)
    for i in range(OUT_STEPS):
        project(i, terms, half + 64, 64, COLS)
    r = lax.broadcasted_iota(jnp.int32, (COLS, COLS), 0)
    c = lax.broadcasted_iota(jnp.int32, (COLS, COLS), 1)
    r_ref[...] = jnp.where(r <= c, work[:, :COLS], 0.0)

    for i in range(OUT_STEPS):
        put(i, 0, half).wait()
        put(i, half, 64).wait()
        put(i, half + 64, 64).wait()


def solve(raw, filt, weight, gathered):
    vmem = pl.BlockSpec(memory_space=pltpu.VMEM)
    hbm = pl.BlockSpec(memory_space=pltpu.HBM)
    return pl.pallas_call(
        solve_kernel,
        out_shape=(jax.ShapeDtypeStruct((COLS, ROWS), jnp.float32), jax.ShapeDtypeStruct((COLS, COLS), jnp.float32)),
        in_specs=[vmem, vmem, vmem, vmem],
        out_specs=(hbm, vmem),
        scratch_shapes=[
            pltpu.VMEM((COLS, 4 * MONTHS), jnp.float32),
            pltpu.VMEM((OUT_STEPS, COLS, OUT_CHUNK), jnp.float32),
            pltpu.SemaphoreType.DMA((4, OUT_STEPS)),
        ],
        compiler_params=pltpu.CompilerParams(vmem_limit_bytes=16 * 1024 * 1024),
        name="solve",
    )(raw, filt, weight, gathered)


def gather_kernel(
    field_ref, weight_in, response_in, table_in, f_ref, g_ref, filt_ref, weight_ref,
    response_ref, table_ref, fbuf, gacc, pieces, pbuf, hbuf, s1buf, s2buf, tbuf,
    phase, own_sem, a_send, a_recv, p_send, p_recv, s1_send, s1_recv, s2_send, s2_recv, s3_send, s3_recv,
):
    core = lax.axis_index("grp")
    me = lax.axis_index("blk")
    my = me // PLANE
    mz = (me // NX) % NZ
    mx = me % NX
    mxy = my * NX + mx
    other = 1 - core

    def at(y, z, x):
        return (y % NY) * PLANE + (z % NZ) * NX + x % NX

    def xy_peer(p):
        return at(p // NX, mz, p % NX)

    def signal(sem, **where):
        pl.semaphore_signal(sem, inc=1, device_id=where)

    def slot_of(p):
        return p // PLANE * PLANE + p % NX * NZ + p // NX % NZ

    def cut(p):
        return field_ref.at[:, aligned(p * ROWS, ROWS)]

    def copy(p, source):
        slot = slot_of(source)
        return pltpu.make_async_remote_copy(
            src_ref=cut(p), dst_ref=fbuf.at[slot], send_sem=a_send.at[p], recv_sem=a_recv.at[slot],
            device_id={"blk": p})

    barrier = pltpu.get_barrier_semaphore()
    for k in range(1, NZ):
        signal(barrier, blk=at(my, mz + k, mx))
    for k in range(1, NX):
        signal(barrier, blk=at(my, mz, mx + k))
    for k in range(1, NY):
        signal(barrier, blk=at(my + k, mz, mx))
    signal(barrier, grp=other)
    pl.semaphore_wait(barrier, NZ + NX + NY - 2)
    for k in range(1, NX):
        signal(phase.at[0], blk=at(my, mz, mx + k))

    def send_line(i, _):
        copy(at(my, mz + i, mx), me).start()
        return 0

    lax.fori_loop(1, NZ, send_line, 0)
    local = [
        pltpu.make_async_copy(cut(me), fbuf.at[slot_of(me)], own_sem.at[0]),
        pltpu.make_async_copy(weight_in, weight_ref, own_sem.at[1]),
        pltpu.make_async_copy(response_in, response_ref, own_sem.at[2]),
        pltpu.make_async_copy(table_in, table_ref, own_sem.at[3]),
    ]
    for each in local:
        each.start()
    pl.semaphore_wait(phase.at[0], NX - 1)
    for k in range(1, NY):
        signal(phase.at[1], blk=at(my + k, mz, mx))

    def send_plane(i, _):
        copy(at(my, mz + 4 + (i % NZ) * 3, mx + 1 + i // NZ), me).start()
        return 0

    lax.fori_loop(0, PLANE - NZ, send_plane, 0)
    pl.semaphore_wait(phase.at[1], NY - 1)

    def send_rest(i, _):
        copy(at(my + 1 + i // PLANE, mz + 4 + (i % NZ) * 3, mx + (i // NZ) % NX), me).start()
        return 0

    lax.fori_loop(0, NB - PLANE, send_rest, 0)

    f_ref[...] = jnp.zeros_like(f_ref)
    for each in local:
        each.wait()
    gain = response_ref[...]
    filt_ref[...] = (
        dot_t(table_ref[2] * gain, table_ref[0], TOP) + dot_t(table_ref[3] * gain, table_ref[1], TOP))

    share = GROUP // 2
    owner_group = (my + 1) % NY

    def pair(t, group):
        return pltpu.make_async_remote_copy(
            src_ref=gacc.at[aligned(group * GROUP + other * share, share)], dst_ref=pbuf.at[t],
            send_sem=p_send.at[t], recv_sem=p_recv.at[t], device_id={"grp": other})

    def s1(t, i, group, slot):
        return pltpu.make_async_remote_copy(
            src_ref=hbuf.at[t, aligned(i * 8, 8)], dst_ref=s1buf.at[slot], send_sem=s1_send.at[t * NX + i],
            recv_sem=s1_recv.at[slot], device_id={"blk": at(group + NY - 1, mz, i)})

    def s1_from(p):
        return pltpu.make_async_remote_copy(
            src_ref=hbuf.at[0, aligned(0, 8)], dst_ref=s1buf.at[p], send_sem=s1_send.at[0],
            recv_sem=s1_recv.at[p], device_id={"blk": xy_peer(p)})

    def window(t):
        group = (my + NY - t) % NY

        def batch(q, _):
            x = (mx + NX - q) % NX

            def arrive(i, _):
                p = at(group, mz + i, x)
                copy(p, p).wait_recv()
                return 0

            lax.fori_loop(jnp.where(t + q == 0, 1, 0), NZ, arrive, 0)
            start = x * BLOCK

            def unpack(c, _):
                lanes = aligned(c * CHUNK, CHUNK)
                block = fbuf[aligned(group * PLANE + x * NZ, NZ), :, lanes].reshape(BLOCK, CHUNK)
                f_ref[aligned(group * GROUP + start, BLOCK), lanes] = block
                w = weight_ref[:, lanes]
                for k, part in enumerate(split3(block.astype(jnp.float32) * (w * w))):
                    pieces[aligned(k * GROUP + start, BLOCK), lanes] = part
                return 0

            lax.fori_loop(0, ROWS // CHUNK, unpack, 0)
            return 0

        lax.fori_loop(0, NX, batch, 0)
        rows = aligned(group * GROUP, GROUP)
        terms = dot_t(pieces[...], f_ref[...])
        total = terms[2 * GROUP:, :] + terms[GROUP:2 * GROUP, :] + terms[:GROUP, :]
        column = lax.broadcasted_iota(jnp.int32, (GROUP, COLS), 1)
        gacc[rows, :] = jnp.where(column // GROUP == group, 0.5 * total, total)
        pair(t, group).start()
        pair(t, group).wait_recv()
        hbuf[t] = gacc[aligned(group * GROUP + core * share, share), :] + pbuf[t]
        return group

    def early(t, _):
        group = window(t)
        for i in range(NX):
            s1(t, i, group, mxy).start()
        return 0

    lax.fori_loop(0, NY - 1, early, 0)
    window(NY - 1)
    row = [(mx + k) % NX for k in range(1, NX)]
    for i in row:
        s1(NY - 1, i, owner_group, mxy).start()

    def s2(p, slot):
        return pltpu.make_async_remote_copy(
            src_ref=tbuf.at[0], dst_ref=s2buf.at[slot], send_sem=s2_send.at[p], recv_sem=s2_recv.at[slot],
            device_id={"blk": at(my, p, mx)})

    def piece(p, c):
        y, x = p // NX, p % NX
        return aligned(((y + 1) % NY) * GROUP + c * share + x * 8, 8)

    def s3(p, c, q, d):
        return pltpu.make_async_remote_copy(
            src_ref=tbuf.at[1], dst_ref=g_ref.at[piece(q, d)],
            send_sem=s3_send.at[c * 16 + p], recv_sem=s3_recv.at[d * 16 + q], device_id={"blk": xy_peer(p), "grp": c})

    xy = [(my + y) % NY * NX + (mx + x) % NX for y, x in FAR_FIRST]
    line = [(mz + k) % NZ for k in (4, 3, 5, 2, 6, 1, 7)]
    total = hbuf[NY - 1, aligned(mx * 8, 8), :]
    for k in range(1, NY):
        for j in range(NX):
            p = (my + k) % NY * NX + j
            s1_from(p).wait_recv()
            total = total + s1buf[p]
    for i in row:
        p = my * NX + i
        s1_from(p).wait_recv()
        total = total + s1buf[p]
    tbuf[0] = total
    s2buf[mz] = total
    for p in line:
        s2(p, mz).start()
    for p in line:
        s2(p, p).wait_recv()
    total = s2buf[0]
    for k in range(1, NZ):
        total = total + s2buf[k]
    tbuf[1] = total
    g_ref[piece(mxy, core), :] = total
    for p in xy:
        s3(p, core, mxy, core).start()
        s3(p, other, mxy, core).start()
    s3(mxy, other, mxy, core).start()
    for p in xy:
        s3(p, core, p, core).wait_recv()
        s3(p, other, p, other).wait_recv()
    s3(mxy, other, mxy, other).wait_recv()
    for p in xy:
        s3(p, core, mxy, core).wait_send()
        s3(p, other, mxy, core).wait_send()
    s3(mxy, other, mxy, core).wait_send()
    for p in line:
        s2(p, p).wait_send()

    def shared(t, _):
        group = (my + NY - t) % NY
        pair(t, group).wait_send()
        for i in range(NX):
            s1(t, i, group, mxy).wait_send()
        return 0

    lax.fori_loop(0, NY - 1, shared, 0)
    pair(NY - 1, owner_group).wait_send()
    for i in row:
        s1(NY - 1, i, owner_group, mxy).wait_send()

    def sent(k, _):
        copy((me + k) % NB, me).wait_send()
        return 0

    lax.fori_loop(1, NB, sent, 0)


def gather_and_gram(field, weight, response, table):
    dma = pltpu.SemaphoreType.DMA
    vmem = pl.BlockSpec(memory_space=pltpu.VMEM)
    hbm = pl.BlockSpec(memory_space=pltpu.HBM)
    return pl.pallas_call(
        gather_kernel,
        out_shape=(
            jax.ShapeDtypeStruct((COLS, ROWS), jnp.bfloat16),
            jax.ShapeDtypeStruct((COLS, COLS), jnp.float32),
            jax.ShapeDtypeStruct((MONTHS, MONTHS), jnp.float32),
            jax.ShapeDtypeStruct((1, ROWS), jnp.float32),
        ),
        in_specs=[hbm, hbm, hbm, hbm],
        out_specs=(vmem, vmem, vmem, vmem),
        scratch_shapes=[
            pltpu.VMEM((1, BINS), jnp.float32),
            pltpu.VMEM((4, MONTHS, BINS), jnp.float32),
            pltpu.VMEM((NB, 2, ROWS), jnp.bfloat16),
            pltpu.VMEM((COLS, COLS), jnp.float32),
            pltpu.VMEM((3 * GROUP, ROWS), jnp.bfloat16),
            pltpu.VMEM((NY, GROUP // 2, COLS), jnp.float32),
            pltpu.VMEM((NY, GROUP // 2, COLS), jnp.float32),
            pltpu.VMEM((16, 8, COLS), jnp.float32),
            pltpu.VMEM((NZ, 8, COLS), jnp.float32),
            pltpu.VMEM((2, 8, COLS), jnp.float32),
            pltpu.SemaphoreType.REGULAR((2,)),
            dma((4,)), dma((NB,)), dma((NB,)), dma((NY,)), dma((NY,)),
            dma((16,)), dma((16,)), dma((NZ,)), dma((NZ,)), dma((32,)), dma((32,)),
        ],
        compiler_params=pltpu.CompilerParams(
            collective_id=0, has_side_effects=True, vmem_limit_bytes=16 * 1024 * 1024),
        name="gather_gram",
    )(field, weight, response, table)


def shards(field, response, area_weight):
    gathered, raw, filt, weight = gather_and_gram(
        *(pltpu.with_memory_space_constraint(x, pltpu.HBM) for x in (field, area_weight.reshape(1, ROWS), response.reshape(1, BINS), jnp.asarray(filter_tables()))))
    return solve(raw, filt, weight, gathered)


def solution(mesh):
    in_specs = (P("blk", "grp"), P(), P(("grp", "blk")))
    out_specs = (P(None, ("grp", "blk")), P())
    return jax.shard_map(shards, mesh=mesh, in_specs=in_specs, out_specs=out_specs, check_vma=False)
```

```python
import jax
import jax.numpy as jnp
import numpy as np
from jax import lax
from jax.experimental import pallas as pl
from jax.experimental.pallas import tpu as pltpu
from jax.sharding import PartitionSpec as P

MONTHS = 128
COLS = 256
BINS = MONTHS // 2 + 1
ROWS = 4096
POINTS = 1048576
TOP = lax.Precision.HIGHEST
NY, NZ, NX = 4, 8, 4
NB = NY * NZ * NX
PLANE = NZ * NX
GROUP = 2 * PLANE
CHUNK = 1024
BLOCK = 16
WIDE = 384
OUT_CHUNK = 512
OUT_STEPS = ROWS // OUT_CHUNK
FAR_FIRST = sorted(((y, x) for y in range(NY) for x in range(NX) if y or x), key=lambda s: -min(s[0], NY - s[0]) - min(s[1], NX - s[1]))


def filter_tables():
    freq = np.arange(BINS)
    edge = (freq == 0) | (freq == MONTHS // 2)
    coef = np.where(edge, 1.0, 2.0) / MONTHS
    angle = 2.0 * np.pi * ((np.arange(MONTHS)[:, None] * freq[None, :]) % MONTHS) / MONTHS
    cos, sin = np.cos(angle), np.sin(angle)
    order = np.arange(MONTHS).reshape(-1, NZ, NX, 2).transpose(0, 2, 1, 3).reshape(-1)
    return np.stack([cos[order], sin[order], cos * coef, sin * coef]).astype(np.float32)


def split3(value):
    high = value.astype(jnp.bfloat16)
    rest = value - high.astype(jnp.float32)
    middle = rest.astype(jnp.bfloat16)
    low = (rest - middle.astype(jnp.float32)).astype(jnp.bfloat16)
    return high, middle, low


def dot_t(a, b, precision=None):
    return lax.dot_general(a, b, (((1,), (1,)), ((), ())), precision=precision, preferred_element_type=jnp.float32)


def aligned(start, n):
    return pl.ds(pl.multiple_of(start, n), n)


def row_of(tile, s):
    return jnp.broadcast_to(tile[s:s + 1, :], (8, 128))


def eliminate(work, b):
    sub = lax.broadcasted_iota(jnp.int32, (8, 128), 0)
    r0 = b * BLOCK
    base = 0 if r0 < MONTHS else MONTHS
    lane = r0 - base
    top = [work[r0:r0 + 8, base + 128 * t:base + 128 * t + 128] for t in range(3)]
    bot = [work[r0 + 8:r0 + 16, base + 128 * t:base + 128 * t + 128] for t in range(3)]
    ct = [jnp.broadcast_to(top[0][:, lane + j:lane + j + 1], (8, 128)) for j in range(8)]
    cb = [jnp.broadcast_to(bot[0][:, lane + j:lane + j + 1], (8, 128)) for j in range(16)]
    for j in range(BLOCK):
        if j < 8:
            d = lax.rsqrt(row_of(ct[j], j))
            lt = ct[j] * d
            lb = cb[j] * d
            for k in range(j + 1, 8):
                f = row_of(ct[j], k) * d if k == j + 1 else row_of(lt, k)
                ct[k] = ct[k] - lt * f
                cb[k] = cb[k] - lb * f
            for k in range(8, 16):
                cb[k] = cb[k] - lb * row_of(lb, k - 8)
            lt = jnp.where(sub > j, lt, 0.0)
            for t in range(3):
                u = row_of(top[t], j) * d
                bot[t] = bot[t] - lb * u
                top[t] = jnp.where(sub == j, u, top[t] - lt * u)
        else:
            i = j - 8
            d = lax.rsqrt(row_of(cb[j], i))
            lb = cb[j] * d
            for k in range(j + 1, 16):
                cb[k] = cb[k] - lb * (row_of(cb[j], k - 8) * d if k == j + 1 else row_of(lb, k - 8))
            lb = jnp.where(sub > i, lb, 0.0)
            for t in range(3):
                u = row_of(bot[t], i) * d
                bot[t] = jnp.where(sub == i, u, bot[t] - lb * u)
    for t in range(3):
        work[r0:r0 + 8, base + 128 * t:base + 128 * t + 128] = top[t]
        work[r0 + 8:r0 + 16, base + 128 * t:base + 128 * t + 128] = bot[t]
    nxt = r0 + BLOCK
    if nxt == COLS:
        return
    panel = jnp.concatenate([jnp.concatenate(top, axis=1), jnp.concatenate(bot, axis=1)], axis=0)
    h, m, l = split3(panel)
    first = nxt // 128 * 128
    left = first - base
    width = COLS - first
    cut = lambda x: x[:, left:left + width]
    a = jnp.concatenate([cut(h), cut(h), cut(m), cut(h), cut(l), cut(m)], axis=0)
    c = jnp.concatenate([h, m, h, l, h, m], axis=0)
    a = a.T
    skip = nxt - first
    for start, stop in ((nxt, nxt + BLOCK), (nxt + BLOCK, COLS)):
        if start < stop:
            prod = jnp.dot(a[start - first:stop - first], c, preferred_element_type=jnp.float32)
            work[start:stop, base:base + WIDE] = work[start:stop, base:base + WIDE] - prod


def solve_kernel(raw_ref, filt_ref, weight_ref, f_ref, out_ref, r_ref, work, obuf, rbuf, osem, rsem):
    mix = filt_ref[...]
    half = MONTHS

    def fold(i, j):
        first = raw_ref[i * half:(i + 1) * half, j * half:(j + 1) * half]
        second = raw_ref[j * half:(j + 1) * half, i * half:(i + 1) * half]
        return (first + second.T) * (1.0 / POINTS)

    zero = jnp.zeros((half, half), jnp.float32)
    sides = [dot_t(fold(0, 0), mix, TOP), dot_t(fold(0, 1), mix, TOP)]
    for rows in (slice(0, BLOCK), slice(BLOCK, half)):
        for k, right in enumerate(sides):
            work[rows, k * half:(k + 1) * half] = jnp.dot(
                mix[rows], right, precision=TOP, preferred_element_type=jnp.float32)
    last = dot_t(fold(1, 1), mix, TOP)
    work[half:, half:2 * half] = jnp.dot(mix, last, precision=TOP, preferred_element_type=jnp.float32)
    work[half:, :half] = zero
    work[:half, 2 * half:3 * half] = mix
    work[:half, 3 * half:] = zero
    work[half:, 2 * half:3 * half] = zero
    work[half:, 3 * half:] = mix

    def put(i, first, count):
        return pltpu.make_async_copy(
            obuf.at[i, pl.ds(first, count)], out_ref.at[pl.ds(first, count), pl.ds(i * OUT_CHUNK, OUT_CHUNK)],
            osem.at[first // 64, i])

    def stacked(first, count, depth):
        return jnp.concatenate(split3(work[first:first + count, 2 * half:2 * half + depth]), axis=0)

    def project(i, terms, first, count, depth):
        lanes = pl.ds(i * OUT_CHUNK, OUT_CHUNK)
        parts = jnp.dot(terms, f_ref[:depth, lanes], preferred_element_type=jnp.float32)
        total = parts[2 * count:] + parts[count:2 * count] + parts[:count]
        obuf[i, first:first + count, :] = total * weight_ref[:, lanes]
        put(i, first, count).start()

    for b in range(8):
        eliminate(work, b)
    terms = stacked(0, half, half)
    for b in range(8, 12):
        eliminate(work, b)
        for i in (2 * b - 16, 2 * b - 15):
            project(i, terms, 0, half, half)
    terms = stacked(half, 64, COLS)
    for b in range(12, 16):
        eliminate(work, b)
        for i in (2 * b - 24, 2 * b - 23):
            project(i, terms, half, 64, COLS)
    r = lax.broadcasted_iota(jnp.int32, (COLS, COLS), 0)
    c = lax.broadcasted_iota(jnp.int32, (COLS, COLS), 1)
    rbuf[...] = jnp.where(r <= c, work[:, :COLS], 0.0)
    triangle = pltpu.make_async_copy(rbuf, r_ref, rsem)
    triangle.start()
    terms = stacked(half + 64, 64, COLS)
    for i in range(OUT_STEPS):
        project(i, terms, half + 64, 64, COLS)
    triangle.wait()
    for i in range(OUT_STEPS):
        put(i, 0, half).wait()
        put(i, half, 64).wait()
        put(i, half + 64, 64).wait()


def solve(raw, filt, weight, gathered):
    vmem = pl.BlockSpec(memory_space=pltpu.VMEM)
    hbm = pl.BlockSpec(memory_space=pltpu.HBM)
    return pl.pallas_call(
        solve_kernel,
        out_shape=(jax.ShapeDtypeStruct((COLS, ROWS), jnp.float32), jax.ShapeDtypeStruct((COLS, COLS), jnp.float32)),
        in_specs=[vmem, vmem, vmem, vmem],
        out_specs=(hbm, hbm),
        scratch_shapes=[
            pltpu.VMEM((COLS, 4 * MONTHS), jnp.float32),
            pltpu.VMEM((OUT_STEPS, COLS, OUT_CHUNK), jnp.float32),
            pltpu.VMEM((COLS, COLS), jnp.float32),
            pltpu.SemaphoreType.DMA((4, OUT_STEPS)),
            pltpu.SemaphoreType.DMA,
        ],
        compiler_params=pltpu.CompilerParams(vmem_limit_bytes=16 * 1024 * 1024),
        name="solve",
    )(raw, filt, weight, gathered)


def gather_kernel(
    field_ref, weight_in, response_in, table_in, f_ref, g_ref, filt_ref, weight_ref,
    response_ref, table_ref, fbuf, gacc, pieces, pbuf, hbuf, s1buf, s2buf, tbuf,
    phase, own_sem, a_send, a_recv, p_send, p_recv, s1_send, s1_recv, s2_send, s2_recv, s3_send, s3_recv,
):
    core = lax.axis_index("grp")
    me = lax.axis_index("blk")
    my = me // PLANE
    mz = (me // NX) % NZ
    mx = me % NX
    mxy = my * NX + mx
    other = 1 - core

    def at(y, z, x):
        return (y % NY) * PLANE + (z % NZ) * NX + x % NX

    def xy_peer(p):
        return at(p // NX, mz, p % NX)

    def signal(sem, **where):
        pl.semaphore_signal(sem, inc=1, device_id=where)

    def slot_of(p):
        return p // PLANE * PLANE + p % NX * NZ + p // NX % NZ

    def cut(p):
        return field_ref.at[:, aligned(p * ROWS, ROWS)]

    def copy(p, source):
        slot = slot_of(source)
        return pltpu.make_async_remote_copy(
            src_ref=cut(p), dst_ref=fbuf.at[slot], send_sem=a_send.at[p], recv_sem=a_recv.at[slot],
            device_id={"blk": p})

    barrier = pltpu.get_barrier_semaphore()
    for k in range(1, NZ):
        signal(barrier, blk=at(my, mz + k, mx))
    for k in range(1, NX):
        signal(barrier, blk=at(my, mz, mx + k))
    for k in range(1, NY):
        signal(barrier, blk=at(my + k, mz, mx))
    signal(barrier, grp=other)
    pl.semaphore_wait(barrier, NZ + NX + NY - 2)
    for k in range(1, NX):
        signal(phase.at[0], blk=at(my, mz, mx + k))

    def far(i):
        return 4 + (i // 2) * (1 - i % 2) - ((i + 1) // 2) * (i % 2) + NZ

    def send_line(i, _):
        copy(at(my, mz + i, mx), me).start()
        return 0

    lax.fori_loop(1, NZ, send_line, 0)
    local = [
        pltpu.make_async_copy(cut(me), fbuf.at[slot_of(me)], own_sem.at[0]),
        pltpu.make_async_copy(weight_in, weight_ref, own_sem.at[1]),
        pltpu.make_async_copy(response_in, response_ref, own_sem.at[2]),
        pltpu.make_async_copy(table_in, table_ref, own_sem.at[3]),
    ]
    for each in local:
        each.start()
    pl.semaphore_wait(phase.at[0], NX - 1)
    for k in range(1, NY):
        signal(phase.at[1], blk=at(my + k, mz, mx))

    def send_plane(i, _):
        copy(at(my, mz + far(i % NZ), mx + 1 + i // NZ), me).start()
        return 0

    lax.fori_loop(0, PLANE - NZ, send_plane, 0)
    pl.semaphore_wait(phase.at[1], NY - 1)

    def send_rest(i, _):
        copy(at(my + 1 + i // PLANE, mz + far(i % NZ), mx + (i // NZ) % NX), me).start()
        return 0

    lax.fori_loop(0, NB - PLANE, send_rest, 0)

    f_ref[...] = jnp.zeros_like(f_ref)
    for each in local:
        each.wait()
    gain = response_ref[...]
    filt_ref[...] = (
        dot_t(table_ref[2] * gain, table_ref[0], TOP) + dot_t(table_ref[3] * gain, table_ref[1], TOP))

    share = GROUP // 2
    owner_group = (my + 1) % NY

    def pair(t, group):
        return pltpu.make_async_remote_copy(
            src_ref=gacc.at[aligned(group * GROUP + other * share, share)], dst_ref=pbuf.at[t],
            send_sem=p_send.at[t], recv_sem=p_recv.at[t], device_id={"grp": other})

    def s1(t, i, group, slot):
        return pltpu.make_async_remote_copy(
            src_ref=hbuf.at[t, aligned(i * 8, 8)], dst_ref=s1buf.at[slot], send_sem=s1_send.at[t * NX + i],
            recv_sem=s1_recv.at[slot], device_id={"blk": at(group + NY - 1, mz, i)})

    def s1_from(p):
        return pltpu.make_async_remote_copy(
            src_ref=hbuf.at[0, aligned(0, 8)], dst_ref=s1buf.at[p], send_sem=s1_send.at[0],
            recv_sem=s1_recv.at[p], device_id={"blk": xy_peer(p)})

    def window(t):
        group = (my + NY - t) % NY

        def batch(q, _):
            x = (mx + NX - q) % NX

            def arrive(i, _):
                p = at(group, mz + i, x)
                copy(p, p).wait_recv()
                return 0

            lax.fori_loop(jnp.where(t + q == 0, 1, 0), NZ, arrive, 0)
            start = x * BLOCK

            def unpack(c, _):
                lanes = aligned(c * CHUNK, CHUNK)
                block = fbuf[aligned(group * PLANE + x * NZ, NZ), :, lanes].reshape(BLOCK, CHUNK)
                f_ref[aligned(group * GROUP + start, BLOCK), lanes] = block
                w = weight_ref[:, lanes]
                for k, part in enumerate(split3(block.astype(jnp.float32) * (w * w))):
                    pieces[aligned(k * GROUP + start, BLOCK), lanes] = part
                return 0

            lax.fori_loop(0, ROWS // CHUNK, unpack, 0)
            return 0

        lax.fori_loop(0, NX, batch, 0)
        rows = aligned(group * GROUP, GROUP)
        terms = dot_t(pieces[...], f_ref[...])
        total = terms[2 * GROUP:, :] + terms[GROUP:2 * GROUP, :] + terms[:GROUP, :]
        column = lax.broadcasted_iota(jnp.int32, (GROUP, COLS), 1)
        gacc[rows, :] = jnp.where(column // GROUP == group, 0.5 * total, total)
        pair(t, group).start()
        pair(t, group).wait_recv()
        hbuf[t] = gacc[aligned(group * GROUP + core * share, share), :] + pbuf[t]
        return group

    def early(t, _):
        group = window(t)
        for i in range(NX):
            s1(t, i, group, mxy).start()
        return 0

    lax.fori_loop(0, NY - 1, early, 0)
    window(NY - 1)
    row = [(mx + k) % NX for k in range(1, NX)]
    for i in row:
        s1(NY - 1, i, owner_group, mxy).start()

    def s2(p, slot):
        return pltpu.make_async_remote_copy(
            src_ref=tbuf.at[0], dst_ref=s2buf.at[slot], send_sem=s2_send.at[p], recv_sem=s2_recv.at[slot],
            device_id={"blk": at(my, p, mx)})

    def piece(p, c):
        y, x = p // NX, p % NX
        return aligned(((y + 1) % NY) * GROUP + c * share + x * 8, 8)

    def s3(p, c, q, d):
        return pltpu.make_async_remote_copy(
            src_ref=tbuf.at[1], dst_ref=g_ref.at[piece(q, d)],
            send_sem=s3_send.at[c * 16 + p], recv_sem=s3_recv.at[d * 16 + q], device_id={"blk": xy_peer(p), "grp": c})

    xy = [(my + y) % NY * NX + (mx + x) % NX for y, x in FAR_FIRST]
    line = [(mz + k) % NZ for k in (4, 3, 5, 2, 6, 1, 7)]
    total = hbuf[NY - 1, aligned(mx * 8, 8), :]
    for k in range(1, NY):
        for j in range(NX):
            p = (my + k) % NY * NX + j
            s1_from(p).wait_recv()
            total = total + s1buf[p]
    for i in row:
        p = my * NX + i
        s1_from(p).wait_recv()
        total = total + s1buf[p]
    tbuf[0] = total
    s2buf[mz] = total
    for p in line:
        s2(p, mz).start()

    def sent(k, _):
        copy((me + k) % NB, me).wait_send()
        return 0

    lax.fori_loop(1, NB, sent, 0)

    def shared(t, _):
        group = (my + NY - t) % NY
        pair(t, group).wait_send()
        for i in range(NX):
            s1(t, i, group, mxy).wait_send()
        return 0

    lax.fori_loop(0, NY - 1, shared, 0)
    pair(NY - 1, owner_group).wait_send()
    for i in row:
        s1(NY - 1, i, owner_group, mxy).wait_send()

    for p in line:
        s2(p, p).wait_recv()
    total = s2buf[0]
    for k in range(1, NZ):
        total = total + s2buf[k]
    tbuf[1] = total
    g_ref[piece(mxy, core), :] = total
    for p in xy:
        s3(p, core, mxy, core).start()
        s3(p, other, mxy, core).start()
    s3(mxy, other, mxy, core).start()
    for p in xy:
        s3(p, core, p, core).wait_recv()
        s3(p, other, p, other).wait_recv()
    s3(mxy, other, mxy, other).wait_recv()
    for p in xy:
        s3(p, core, mxy, core).wait_send()
        s3(p, other, mxy, core).wait_send()
    s3(mxy, other, mxy, core).wait_send()
    for p in line:
        s2(p, p).wait_send()


def gather_and_gram(field, weight, response, table):
    dma = pltpu.SemaphoreType.DMA
    vmem = pl.BlockSpec(memory_space=pltpu.VMEM)
    hbm = pl.BlockSpec(memory_space=pltpu.HBM)
    return pl.pallas_call(
        gather_kernel,
        out_shape=(
            jax.ShapeDtypeStruct((COLS, ROWS), jnp.bfloat16),
            jax.ShapeDtypeStruct((COLS, COLS), jnp.float32),
            jax.ShapeDtypeStruct((MONTHS, MONTHS), jnp.float32),
            jax.ShapeDtypeStruct((1, ROWS), jnp.float32),
        ),
        in_specs=[hbm, hbm, hbm, hbm],
        out_specs=(vmem, vmem, vmem, vmem),
        scratch_shapes=[
            pltpu.VMEM((1, BINS), jnp.float32),
            pltpu.VMEM((4, MONTHS, BINS), jnp.float32),
            pltpu.VMEM((NB, 2, ROWS), jnp.bfloat16),
            pltpu.VMEM((COLS, COLS), jnp.float32),
            pltpu.VMEM((3 * GROUP, ROWS), jnp.bfloat16),
            pltpu.VMEM((NY, GROUP // 2, COLS), jnp.float32),
            pltpu.VMEM((NY, GROUP // 2, COLS), jnp.float32),
            pltpu.VMEM((16, 8, COLS), jnp.float32),
            pltpu.VMEM((NZ, 8, COLS), jnp.float32),
            pltpu.VMEM((2, 8, COLS), jnp.float32),
            pltpu.SemaphoreType.REGULAR((2,)),
            dma((4,)), dma((NB,)), dma((NB,)), dma((NY,)), dma((NY,)),
            dma((16,)), dma((16,)), dma((NZ,)), dma((NZ,)), dma((32,)), dma((32,)),
        ],
        compiler_params=pltpu.CompilerParams(
            collective_id=0, has_side_effects=True, vmem_limit_bytes=16 * 1024 * 1024),
        name="gather_gram",
    )(field, weight, response, table)


def shards(field, response, area_weight):
    gathered, raw, filt, weight = gather_and_gram(
        *(pltpu.with_memory_space_constraint(x, pltpu.HBM) for x in (field, area_weight.reshape(1, ROWS), response.reshape(1, BINS), jnp.asarray(filter_tables()))))
    return solve(raw, filt, weight, gathered)


def solution(mesh):
    in_specs = (P("blk", "grp"), P(), P(("grp", "blk")))
    out_specs = (P(None, ("grp", "blk")), P())
    return jax.shard_map(shards, mesh=mesh, in_specs=in_specs, out_specs=out_specs, check_vma=False)
```

```python
import jax
import jax.numpy as jnp
import numpy as np
from jax import lax
from jax.experimental import pallas as pl
from jax.experimental.pallas import tpu as pltpu
from jax.sharding import PartitionSpec as P

MONTHS = 128
COLS = 256
BINS = MONTHS // 2 + 1
ROWS = 4096
POINTS = 1048576
TOP = lax.Precision.HIGHEST
NY, NZ, NX = 4, 8, 4
NB = NY * NZ * NX
PLANE = NZ * NX
GROUP = 2 * PLANE
CHUNK = 1024
BLOCK = 16
WIDE = 384
OUT_CHUNK = 1024
OUT_STEPS = ROWS // OUT_CHUNK
FAR_FIRST = sorted(((y, x) for y in range(NY) for x in range(NX) if y or x), key=lambda s: -min(s[0], NY - s[0]) - min(s[1], NX - s[1]))


def filter_tables():
    freq = np.arange(BINS)
    edge = (freq == 0) | (freq == MONTHS // 2)
    coef = np.where(edge, 1.0, 2.0) / MONTHS
    angle = 2.0 * np.pi * ((np.arange(MONTHS)[:, None] * freq[None, :]) % MONTHS) / MONTHS
    cos, sin = np.cos(angle), np.sin(angle)
    order = np.arange(MONTHS).reshape(-1, NZ, NX, 2).transpose(0, 2, 1, 3).reshape(-1)
    return np.stack([cos[order], sin[order], cos * coef, sin * coef]).astype(np.float32)


def split3(value):
    high = value.astype(jnp.bfloat16)
    rest = value - high.astype(jnp.float32)
    middle = rest.astype(jnp.bfloat16)
    low = (rest - middle.astype(jnp.float32)).astype(jnp.bfloat16)
    return high, middle, low


def dot_t(a, b, precision=None):
    return lax.dot_general(a, b, (((1,), (1,)), ((), ())), precision=precision, preferred_element_type=jnp.float32)


def aligned(start, n):
    return pl.ds(pl.multiple_of(start, n), n)


def row_of(tile, s):
    return jnp.broadcast_to(tile[s:s + 1, :], (8, 128))


def eliminate(work, b):
    sub = lax.broadcasted_iota(jnp.int32, (8, 128), 0)
    r0 = b * BLOCK
    base = 0 if r0 < MONTHS else MONTHS
    lane = r0 - base
    top = [work[r0:r0 + 8, base + 128 * t:base + 128 * t + 128] for t in range(3)]
    bot = [work[r0 + 8:r0 + 16, base + 128 * t:base + 128 * t + 128] for t in range(3)]
    ct = [jnp.broadcast_to(top[0][:, lane + j:lane + j + 1], (8, 128)) for j in range(8)]
    cb = [jnp.broadcast_to(bot[0][:, lane + j:lane + j + 1], (8, 128)) for j in range(16)]
    for j in range(BLOCK):
        if j < 8:
            d = lax.rsqrt(row_of(ct[j], j))
            lt = ct[j] * d
            lb = cb[j] * d
            for k in range(j + 1, 8):
                f = row_of(ct[j], k) * d if k == j + 1 else row_of(lt, k)
                ct[k] = ct[k] - lt * f
                cb[k] = cb[k] - lb * f
            for k in range(8, 16):
                cb[k] = cb[k] - lb * row_of(lb, k - 8)
            lt = jnp.where(sub > j, lt, 0.0)
            for t in range(3):
                u = row_of(top[t], j) * d
                bot[t] = bot[t] - lb * u
                top[t] = jnp.where(sub == j, u, top[t] - lt * u)
        else:
            i = j - 8
            d = lax.rsqrt(row_of(cb[j], i))
            lb = cb[j] * d
            for k in range(j + 1, 16):
                cb[k] = cb[k] - lb * (row_of(cb[j], k - 8) * d if k == j + 1 else row_of(lb, k - 8))
            lb = jnp.where(sub > i, lb, 0.0)
            for t in range(3):
                u = row_of(bot[t], i) * d
                bot[t] = jnp.where(sub == i, u, bot[t] - lb * u)
    for t in range(3):
        work[r0:r0 + 8, base + 128 * t:base + 128 * t + 128] = top[t]
        work[r0 + 8:r0 + 16, base + 128 * t:base + 128 * t + 128] = bot[t]
    nxt = r0 + BLOCK
    if nxt == COLS:
        return
    panel = jnp.concatenate([jnp.concatenate(top, axis=1), jnp.concatenate(bot, axis=1)], axis=0)
    h, m, l = split3(panel)
    first = nxt // 128 * 128
    left = first - base
    width = COLS - first
    cut = lambda x: x[:, left:left + width]
    a = jnp.concatenate([cut(h), cut(h), cut(m), cut(h), cut(l), cut(m)], axis=0)
    c = jnp.concatenate([h, m, h, l, h, m], axis=0)
    a = a.T
    skip = nxt - first
    for start, stop in ((nxt, nxt + BLOCK), (nxt + BLOCK, COLS)):
        if start < stop:
            prod = jnp.dot(a[start - first:stop - first], c, preferred_element_type=jnp.float32)
            work[start:stop, base:base + WIDE] = work[start:stop, base:base + WIDE] - prod


def solve_kernel(raw_ref, filt_ref, weight_ref, f_ref, out_ref, r_ref, work, obuf, rbuf, osem, rsem):
    mix = filt_ref[...]
    half = MONTHS

    def fold(i, j):
        first = raw_ref[i * half:(i + 1) * half, j * half:(j + 1) * half]
        second = raw_ref[j * half:(j + 1) * half, i * half:(i + 1) * half]
        return (first + second.T) * (1.0 / POINTS)

    zero = jnp.zeros((half, half), jnp.float32)
    def six(value, left, axis):
        h, m, l = split3(value)
        return jnp.concatenate([h, h, m, h, l, m] if left else [h, m, h, l, h, m], axis=axis)

    wide = six(mix, True, 1)
    product = lambda rows, right: jnp.dot(rows, six(right, False, 0), preferred_element_type=jnp.float32)
    sides = [dot_t(six(fold(0, k), False, 1), wide) for k in range(2)]
    for rows in (slice(0, BLOCK), slice(BLOCK, half)):
        for k, right in enumerate(sides):
            work[rows, k * half:(k + 1) * half] = product(wide[rows], right)
    work[half:, half:2 * half] = product(wide, dot_t(six(fold(1, 1), False, 1), wide))
    work[half:, :half] = zero
    work[:half, 2 * half:3 * half] = mix
    work[:half, 3 * half:] = zero
    work[half:, 2 * half:3 * half] = zero
    work[half:, 3 * half:] = mix

    def put(i, first, count):
        return pltpu.make_async_copy(
            obuf.at[i, pl.ds(first, count)], out_ref.at[pl.ds(first, count), pl.ds(i * OUT_CHUNK, OUT_CHUNK)],
            osem.at[first // 64, i])

    def stacked(first, count, depth):
        return jnp.concatenate(split3(work[first:first + count, 2 * half:2 * half + depth]), axis=0)

    def project(i, terms, first, count, depth):
        lanes = pl.ds(i * OUT_CHUNK, OUT_CHUNK)
        parts = jnp.dot(terms, f_ref[:depth, lanes], preferred_element_type=jnp.float32)
        total = parts[2 * count:] + parts[count:2 * count] + parts[:count]
        obuf[i, first:first + count, :] = total * weight_ref[:, lanes]
        put(i, first, count).start()

    for b in range(8):
        eliminate(work, b)
    terms = stacked(0, half, half)
    for b in range(8, 12):
        eliminate(work, b)
        for i in (b - 8,):
            project(i, terms, 0, half, half)
    terms = stacked(half, 64, COLS)
    for b in range(12, 16):
        eliminate(work, b)
        for i in (b - 12,):
            project(i, terms, half, 64, COLS)
    r = lax.broadcasted_iota(jnp.int32, (COLS, COLS), 0)
    c = lax.broadcasted_iota(jnp.int32, (COLS, COLS), 1)
    rbuf[...] = jnp.where(r <= c, work[:, :COLS], 0.0)
    triangle = pltpu.make_async_copy(rbuf, r_ref, rsem)
    triangle.start()
    terms = stacked(half + 64, 64, COLS)
    for i in range(OUT_STEPS):
        project(i, terms, half + 64, 64, COLS)
    triangle.wait()
    for i in range(OUT_STEPS):
        put(i, 0, half).wait()
        put(i, half, 64).wait()
        put(i, half + 64, 64).wait()


def solve(raw, filt, weight, gathered):
    vmem = pl.BlockSpec(memory_space=pltpu.VMEM)
    hbm = pl.BlockSpec(memory_space=pltpu.HBM)
    return pl.pallas_call(
        solve_kernel,
        out_shape=(jax.ShapeDtypeStruct((COLS, ROWS), jnp.float32), jax.ShapeDtypeStruct((COLS, COLS), jnp.float32)),
        in_specs=[vmem, vmem, vmem, vmem],
        out_specs=(hbm, hbm),
        scratch_shapes=[
            pltpu.VMEM((COLS, 4 * MONTHS), jnp.float32),
            pltpu.VMEM((OUT_STEPS, COLS, OUT_CHUNK), jnp.float32),
            pltpu.VMEM((COLS, COLS), jnp.float32),
            pltpu.SemaphoreType.DMA((4, OUT_STEPS)),
            pltpu.SemaphoreType.DMA,
        ],
        compiler_params=pltpu.CompilerParams(vmem_limit_bytes=16 * 1024 * 1024),
        name="solve",
    )(raw, filt, weight, gathered)


def gather_kernel(
    field_ref, weight_in, response_in, table_in, f_ref, g_ref, filt_ref, weight_ref,
    response_ref, table_ref, fbuf, gacc, pieces, pbuf, hbuf, s1buf, s2buf, tbuf,
    phase, own_sem, a_send, a_recv, p_send, p_recv, s1_send, s1_recv, s2_send, s2_recv, s3_send, s3_recv,
):
    core = lax.axis_index("grp")
    me = lax.axis_index("blk")
    my = me // PLANE
    mz = (me // NX) % NZ
    mx = me % NX
    mxy = my * NX + mx
    other = 1 - core

    def at(y, z, x):
        return (y % NY) * PLANE + (z % NZ) * NX + x % NX

    def xy_peer(p):
        return at(p // NX, mz, p % NX)

    def signal(sem, **where):
        pl.semaphore_signal(sem, inc=1, device_id=where)

    def slot_of(p):
        return p // PLANE * PLANE + p % NX * NZ + p // NX % NZ

    def cut(p):
        return field_ref.at[:, aligned(p * ROWS, ROWS)]

    def copy(p, source):
        slot = slot_of(source)
        return pltpu.make_async_remote_copy(
            src_ref=cut(p), dst_ref=fbuf.at[slot], send_sem=a_send.at[p], recv_sem=a_recv.at[slot],
            device_id={"blk": p})

    barrier = pltpu.get_barrier_semaphore()
    for k in (4, 3, 5, 2, 6, 1, 7):
        signal(barrier, blk=at(my, mz + k, mx))
    for k in range(1, NX):
        signal(barrier, blk=at(my, mz, mx + k))
    for k in range(1, NY):
        signal(barrier, blk=at(my + k, mz, mx))
    signal(barrier, grp=other)
    pl.semaphore_wait(barrier, NZ + NX + NY - 2)
    for k in range(1, NX):
        signal(phase.at[0], blk=at(my, mz, mx + k))

    def far(i):
        return 4 + (i // 2) * (1 - i % 2) - ((i + 1) // 2) * (i % 2) + NZ

    def send_line(i, _):
        copy(at(my, mz + far(i), mx), me).start()
        return 0

    lax.fori_loop(0, NZ - 1, send_line, 0)
    local = [
        pltpu.make_async_copy(cut(me), fbuf.at[slot_of(me)], own_sem.at[0]),
        pltpu.make_async_copy(weight_in, weight_ref, own_sem.at[1]),
        pltpu.make_async_copy(response_in, response_ref, own_sem.at[2]),
        pltpu.make_async_copy(table_in, table_ref, own_sem.at[3]),
    ]
    for each in local:
        each.start()
    pl.semaphore_wait(phase.at[0], NX - 1)
    for k in range(1, NY):
        signal(phase.at[1], blk=at(my + k, mz, mx))

    def send_plane(i, _):
        copy(at(my, mz + far(i % NZ), mx + 1 + i // NZ), me).start()
        return 0

    lax.fori_loop(0, PLANE - NZ, send_plane, 0)
    pl.semaphore_wait(phase.at[1], NY - 1)

    def send_rest(i, _):
        copy(at(my + 1 + i // PLANE, mz + far(i % NZ), mx + (i // NZ) % NX), me).start()
        return 0

    lax.fori_loop(0, NB - PLANE, send_rest, 0)

    f_ref[...] = jnp.zeros_like(f_ref)
    for each in local:
        each.wait()
    gain = response_ref[...]
    filt_ref[...] = (
        dot_t(table_ref[2] * gain, table_ref[0], TOP) + dot_t(table_ref[3] * gain, table_ref[1], TOP))

    share = GROUP // 2
    owner_group = (my + 1) % NY

    def pair(t, group):
        return pltpu.make_async_remote_copy(
            src_ref=gacc.at[aligned(group * GROUP + other * share, share)], dst_ref=pbuf.at[t],
            send_sem=p_send.at[t], recv_sem=p_recv.at[t], device_id={"grp": other})

    def s1(t, i, group, slot):
        return pltpu.make_async_remote_copy(
            src_ref=hbuf.at[t, aligned(i * 8, 8)], dst_ref=s1buf.at[slot], send_sem=s1_send.at[t * NX + i],
            recv_sem=s1_recv.at[slot], device_id={"blk": at(group + NY - 1, mz, i)})

    def s1_from(p):
        return pltpu.make_async_remote_copy(
            src_ref=hbuf.at[0, aligned(0, 8)], dst_ref=s1buf.at[p], send_sem=s1_send.at[0],
            recv_sem=s1_recv.at[p], device_id={"blk": xy_peer(p)})

    def window(t):
        group = (my + NY - t) % NY

        def batch(q, _):
            x = (mx + NX - q) % NX

            def arrive(i, _):
                p = at(group, mz + i, x)
                copy(p, p).wait_recv()
                return 0

            lax.fori_loop(jnp.where(t + q == 0, 1, 0), NZ, arrive, 0)
            start = x * BLOCK

            def unpack(c, _):
                lanes = aligned(c * CHUNK, CHUNK)
                block = fbuf[aligned(group * PLANE + x * NZ, NZ), :, lanes].reshape(BLOCK, CHUNK)
                f_ref[aligned(group * GROUP + start, BLOCK), lanes] = block
                w = weight_ref[:, lanes]
                for k, part in enumerate(split3(block.astype(jnp.float32) * (w * w))):
                    pieces[aligned(k * GROUP + start, BLOCK), lanes] = part
                return 0

            lax.fori_loop(0, ROWS // CHUNK, unpack, 0)
            return 0

        lax.fori_loop(0, NX, batch, 0)
        rows = aligned(group * GROUP, GROUP)
        terms = dot_t(pieces[...], f_ref[...])
        total = terms[2 * GROUP:, :] + terms[GROUP:2 * GROUP, :] + terms[:GROUP, :]
        column = lax.broadcasted_iota(jnp.int32, (GROUP, COLS), 1)
        gacc[rows, :] = jnp.where(column // GROUP == group, 0.5 * total, total)
        pair(t, group).start()
        pair(t, group).wait_recv()
        hbuf[t] = gacc[aligned(group * GROUP + core * share, share), :] + pbuf[t]
        return group

    def early(t, _):
        group = window(t)
        for i in range(NX):
            s1(t, i, group, mxy).start()
        return 0

    lax.fori_loop(0, NY - 1, early, 0)
    window(NY - 1)
    row = [(mx + k) % NX for k in range(1, NX)]
    for i in row:
        s1(NY - 1, i, owner_group, mxy).start()

    def s2(p, slot):
        return pltpu.make_async_remote_copy(
            src_ref=tbuf.at[0], dst_ref=s2buf.at[slot], send_sem=s2_send.at[p], recv_sem=s2_recv.at[slot],
            device_id={"blk": at(my, p, mx)})

    def piece(p, c):
        y, x = p // NX, p % NX
        return aligned(((y + 1) % NY) * GROUP + c * share + x * 8, 8)

    def s3(p, c, q, d):
        return pltpu.make_async_remote_copy(
            src_ref=tbuf.at[1], dst_ref=g_ref.at[piece(q, d)],
            send_sem=s3_send.at[c * 16 + p], recv_sem=s3_recv.at[d * 16 + q], device_id={"blk": xy_peer(p), "grp": c})

    xy = [(my + y) % NY * NX + (mx + x) % NX for y, x in FAR_FIRST]
    line = [(mz + k) % NZ for k in (4, 3, 5, 2, 6, 1, 7)]
    total = hbuf[NY - 1, aligned(mx * 8, 8), :]
    for k in range(1, NY):
        for j in range(NX):
            p = (my + k) % NY * NX + j
            s1_from(p).wait_recv()
            total = total + s1buf[p]
    for i in row:
        p = my * NX + i
        s1_from(p).wait_recv()
        total = total + s1buf[p]
    tbuf[0] = total
    s2buf[mz] = total
    for p in line:
        s2(p, mz).start()

    def sent(k, _):
        copy((me + k) % NB, me).wait_send()
        return 0

    lax.fori_loop(1, NB, sent, 0)

    def shared(t, _):
        group = (my + NY - t) % NY
        pair(t, group).wait_send()
        for i in range(NX):
            s1(t, i, group, mxy).wait_send()
        return 0

    lax.fori_loop(0, NY - 1, shared, 0)
    pair(NY - 1, owner_group).wait_send()
    for i in row:
        s1(NY - 1, i, owner_group, mxy).wait_send()

    for p in line:
        s2(p, p).wait_recv()
    total = s2buf[0]
    for k in range(1, NZ):
        total = total + s2buf[k]
    tbuf[1] = total
    g_ref[piece(mxy, core), :] = total
    for p in xy:
        s3(p, core, mxy, core).start()
        s3(p, other, mxy, core).start()
    s3(mxy, other, mxy, core).start()
    for p in xy:
        s3(p, core, p, core).wait_recv()
        s3(p, other, p, other).wait_recv()
    s3(mxy, other, mxy, other).wait_recv()
    for p in xy:
        s3(p, core, mxy, core).wait_send()
        s3(p, other, mxy, core).wait_send()
    s3(mxy, other, mxy, core).wait_send()
    for p in line:
        s2(p, p).wait_send()


def gather_and_gram(field, weight, response, table):
    dma = pltpu.SemaphoreType.DMA
    vmem = pl.BlockSpec(memory_space=pltpu.VMEM)
    hbm = pl.BlockSpec(memory_space=pltpu.HBM)
    return pl.pallas_call(
        gather_kernel,
        out_shape=(
            jax.ShapeDtypeStruct((COLS, ROWS), jnp.bfloat16),
            jax.ShapeDtypeStruct((COLS, COLS), jnp.float32),
            jax.ShapeDtypeStruct((MONTHS, MONTHS), jnp.float32),
            jax.ShapeDtypeStruct((1, ROWS), jnp.float32),
        ),
        in_specs=[hbm, hbm, hbm, hbm],
        out_specs=(vmem, vmem, vmem, vmem),
        scratch_shapes=[
            pltpu.VMEM((1, BINS), jnp.float32),
            pltpu.VMEM((4, MONTHS, BINS), jnp.float32),
            pltpu.VMEM((NB, 2, ROWS), jnp.bfloat16),
            pltpu.VMEM((COLS, COLS), jnp.float32),
            pltpu.VMEM((3 * GROUP, ROWS), jnp.bfloat16),
            pltpu.VMEM((NY, GROUP // 2, COLS), jnp.float32),
            pltpu.VMEM((NY, GROUP // 2, COLS), jnp.float32),
            pltpu.VMEM((16, 8, COLS), jnp.float32),
            pltpu.VMEM((NZ, 8, COLS), jnp.float32),
            pltpu.VMEM((2, 8, COLS), jnp.float32),
            pltpu.SemaphoreType.REGULAR((2,)),
            dma((4,)), dma((NB,)), dma((NB,)), dma((NY,)), dma((NY,)),
            dma((16,)), dma((16,)), dma((NZ,)), dma((NZ,)), dma((32,)), dma((32,)),
        ],
        compiler_params=pltpu.CompilerParams(
            collective_id=0, has_side_effects=True, vmem_limit_bytes=16 * 1024 * 1024),
        name="gather_gram",
    )(field, weight, response, table)


def shards(field, response, area_weight):
    gathered, raw, filt, weight = gather_and_gram(
        *(pltpu.with_memory_space_constraint(x, pltpu.HBM) for x in (field, area_weight.reshape(1, ROWS), response.reshape(1, BINS), jnp.asarray(filter_tables()))))
    return solve(raw, filt, weight, gathered)


def solution(mesh):
    in_specs = (P("blk", "grp"), P(), P(("grp", "blk")))
    out_specs = (P(None, ("grp", "blk")), P())
    return jax.shard_map(shards, mesh=mesh, in_specs=in_specs, out_specs=out_specs, check_vma=False)
```

```python
import jax
import jax.numpy as jnp
import numpy as np
from jax import lax
from jax.experimental import pallas as pl
from jax.experimental.pallas import tpu as pltpu
from jax.sharding import PartitionSpec as P

MONTHS = 128
COLS = 256
BINS = MONTHS // 2 + 1
ROWS = 4096
POINTS = 1048576
TOP = lax.Precision.HIGHEST
NY, NZ, NX = 4, 8, 4
NB = NY * NZ * NX
PLANE = NZ * NX
GROUP = 2 * PLANE
CHUNK = 2048
BLOCK = 16
WIDE = 384
OUT_CHUNK = 1024
OUT_STEPS = ROWS // OUT_CHUNK
FAR_FIRST = sorted(((y, x) for y in range(NY) for x in range(NX) if y or x), key=lambda s: -min(s[0], NY - s[0]) - min(s[1], NX - s[1]))


def filter_tables():
    freq = np.arange(BINS)
    edge = (freq == 0) | (freq == MONTHS // 2)
    coef = np.where(edge, 1.0, 2.0) / MONTHS
    angle = 2.0 * np.pi * ((np.arange(MONTHS)[:, None] * freq[None, :]) % MONTHS) / MONTHS
    cos, sin = np.cos(angle), np.sin(angle)
    order = np.arange(MONTHS).reshape(-1, NZ, NX, 2).transpose(0, 2, 1, 3).reshape(-1)
    return np.stack([cos[order], sin[order], cos * coef, sin * coef]).astype(np.float32)


def split3(value):
    high = value.astype(jnp.bfloat16)
    rest = value - high.astype(jnp.float32)
    middle = rest.astype(jnp.bfloat16)
    low = (rest - middle.astype(jnp.float32)).astype(jnp.bfloat16)
    return high, middle, low


def dot_t(a, b, precision=None):
    return lax.dot_general(a, b, (((1,), (1,)), ((), ())), precision=precision, preferred_element_type=jnp.float32)


def aligned(start, n):
    return pl.ds(pl.multiple_of(start, n), n)


def row_of(tile, s):
    return jnp.broadcast_to(tile[s:s + 1, :], (8, 128))


def eliminate(work, b):
    sub = lax.broadcasted_iota(jnp.int32, (8, 128), 0)
    r0 = b * BLOCK
    base = 0 if r0 < MONTHS else MONTHS
    lane = r0 - base
    top = [work[r0:r0 + 8, base + 128 * t:base + 128 * t + 128] for t in range(3)]
    bot = [work[r0 + 8:r0 + 16, base + 128 * t:base + 128 * t + 128] for t in range(3)]
    ct = [jnp.broadcast_to(top[0][:, lane + j:lane + j + 1], (8, 128)) for j in range(8)]
    cb = [jnp.broadcast_to(bot[0][:, lane + j:lane + j + 1], (8, 128)) for j in range(16)]
    for j in range(BLOCK):
        if j < 8:
            d = lax.rsqrt(row_of(ct[j], j))
            lt = ct[j] * d
            lb = cb[j] * d
            for k in range(j + 1, 8):
                f = row_of(ct[j], k) * d if k == j + 1 else row_of(lt, k)
                ct[k] = ct[k] - lt * f
                cb[k] = cb[k] - lb * f
            for k in range(8, 16):
                cb[k] = cb[k] - lb * row_of(lb, k - 8)
            lt = jnp.where(sub > j, lt, 0.0)
            for t in range(3):
                u = row_of(top[t], j) * d
                bot[t] = bot[t] - lb * u
                top[t] = jnp.where(sub == j, u, top[t] - lt * u)
        else:
            i = j - 8
            d = lax.rsqrt(row_of(cb[j], i))
            lb = cb[j] * d
            for k in range(j + 1, 16):
                cb[k] = cb[k] - lb * (row_of(cb[j], k - 8) * d if k == j + 1 else row_of(lb, k - 8))
            lb = jnp.where(sub > i, lb, 0.0)
            for t in range(3):
                u = row_of(bot[t], i) * d
                bot[t] = jnp.where(sub == i, u, bot[t] - lb * u)
    for t in range(3):
        work[r0:r0 + 8, base + 128 * t:base + 128 * t + 128] = top[t]
        work[r0 + 8:r0 + 16, base + 128 * t:base + 128 * t + 128] = bot[t]
    nxt = r0 + BLOCK
    if nxt == COLS:
        return
    panel = jnp.concatenate([jnp.concatenate(top, axis=1), jnp.concatenate(bot, axis=1)], axis=0)
    h, m, l = split3(panel)
    first = nxt // 128 * 128
    left = first - base
    width = COLS - first
    cut = lambda x: x[:, left:left + width]
    a = jnp.concatenate([cut(h), cut(h), cut(m), cut(h), cut(l), cut(m)], axis=0)
    c = jnp.concatenate([h, m, h, l, h, m], axis=0)
    a = a.T
    skip = nxt - first
    for start, stop in ((nxt, nxt + BLOCK), (nxt + BLOCK, COLS)):
        if start < stop:
            prod = jnp.dot(a[start - first:stop - first], c, preferred_element_type=jnp.float32)
            work[start:stop, base:base + WIDE] = work[start:stop, base:base + WIDE] - prod


def solve_kernel(raw_ref, filt_ref, weight_ref, f_ref, out_ref, r_ref, work, obuf, rbuf, osem, rsem):
    mix = filt_ref[...]
    half = MONTHS

    def fold(i, j):
        first = raw_ref[i * half:(i + 1) * half, j * half:(j + 1) * half]
        second = raw_ref[j * half:(j + 1) * half, i * half:(i + 1) * half]
        return (first + second.T) * (1.0 / POINTS)

    zero = jnp.zeros((half, half), jnp.float32)
    def six(value, left, axis):
        h, m, l = split3(value)
        return jnp.concatenate([h, h, m, h, l, m] if left else [h, m, h, l, h, m], axis=axis)

    wide = six(mix, True, 1)
    product = lambda rows, right: jnp.dot(rows, six(right, False, 0), preferred_element_type=jnp.float32)
    sides = [dot_t(six(fold(0, k), False, 1), wide) for k in range(2)]
    for rows in (slice(0, BLOCK), slice(BLOCK, half)):
        for k, right in enumerate(sides):
            work[rows, k * half:(k + 1) * half] = product(wide[rows], right)
    work[half:, half:2 * half] = product(wide, dot_t(six(fold(1, 1), False, 1), wide))
    work[half:, :half] = zero
    work[:half, 2 * half:3 * half] = mix
    work[:half, 3 * half:] = zero
    work[half:, 2 * half:3 * half] = zero
    work[half:, 3 * half:] = mix

    def put(i, first, count):
        return pltpu.make_async_copy(
            obuf.at[i, pl.ds(first, count)], out_ref.at[pl.ds(first, count), pl.ds(i * OUT_CHUNK, OUT_CHUNK)],
            osem.at[first // 64, i])

    def stacked(first, count, depth):
        return jnp.concatenate(split3(work[first:first + count, 2 * half:2 * half + depth]), axis=0)

    def project(i, terms, first, count, depth):
        lanes = pl.ds(i * OUT_CHUNK, OUT_CHUNK)
        parts = jnp.dot(terms, f_ref[:depth, lanes], preferred_element_type=jnp.float32)
        total = parts[2 * count:] + parts[count:2 * count] + parts[:count]
        obuf[i, first:first + count, :] = total * weight_ref[:, lanes]
        put(i, first, count).start()

    for b in range(8):
        eliminate(work, b)
    terms = stacked(0, half, half)
    for b in range(8, 12):
        eliminate(work, b)
        for i in (b - 8,):
            project(i, terms, 0, half, half)
    terms = stacked(half, 64, COLS)
    for b in range(12, 16):
        eliminate(work, b)
        for i in (b - 12,):
            project(i, terms, half, 64, COLS)
    r = lax.broadcasted_iota(jnp.int32, (COLS, COLS), 0)
    c = lax.broadcasted_iota(jnp.int32, (COLS, COLS), 1)
    rbuf[...] = jnp.where(r <= c, work[:, :COLS], 0.0)
    triangle = pltpu.make_async_copy(rbuf, r_ref, rsem)
    triangle.start()
    terms = stacked(half + 64, 64, COLS)
    for i in range(OUT_STEPS):
        project(i, terms, half + 64, 64, COLS)
    triangle.wait()
    for i in range(OUT_STEPS):
        put(i, 0, half).wait()
        put(i, half, 64).wait()
        put(i, half + 64, 64).wait()


def solve(raw, filt, weight, gathered):
    vmem = pl.BlockSpec(memory_space=pltpu.VMEM)
    hbm = pl.BlockSpec(memory_space=pltpu.HBM)
    return pl.pallas_call(
        solve_kernel,
        out_shape=(jax.ShapeDtypeStruct((COLS, ROWS), jnp.float32), jax.ShapeDtypeStruct((COLS, COLS), jnp.float32)),
        in_specs=[vmem, vmem, vmem, vmem],
        out_specs=(hbm, hbm),
        scratch_shapes=[
            pltpu.VMEM((COLS, 4 * MONTHS), jnp.float32),
            pltpu.VMEM((OUT_STEPS, COLS, OUT_CHUNK), jnp.float32),
            pltpu.VMEM((COLS, COLS), jnp.float32),
            pltpu.SemaphoreType.DMA((4, OUT_STEPS)),
            pltpu.SemaphoreType.DMA,
        ],
        compiler_params=pltpu.CompilerParams(vmem_limit_bytes=16 * 1024 * 1024),
        name="solve",
    )(raw, filt, weight, gathered)


def gather_kernel(
    field_ref, weight_in, response_in, table_in, f_ref, g_ref, filt_ref, weight_ref,
    response_ref, table_ref, fbuf, gacc, pieces, pbuf, hbuf, s1buf, s2buf, tbuf,
    phase, own_sem, a_send, a_recv, p_send, p_recv, s1_send, s1_recv, s2_send, s2_recv, s3_send, s3_recv,
):
    core = lax.axis_index("grp")
    me = lax.axis_index("blk")
    my = me // PLANE
    mz = (me // NX) % NZ
    mx = me % NX
    mxy = my * NX + mx
    other = 1 - core

    def at(y, z, x):
        return (y % NY) * PLANE + (z % NZ) * NX + x % NX

    def xy_peer(p):
        return at(p // NX, mz, p % NX)

    def signal(sem, **where):
        pl.semaphore_signal(sem, inc=1, device_id=where)

    def slot_of(p):
        return p // PLANE * PLANE + p % NX * NZ + p // NX % NZ

    def cut(p):
        return field_ref.at[:, aligned(p * ROWS, ROWS)]

    def copy(p, source):
        slot = slot_of(source)
        return pltpu.make_async_remote_copy(
            src_ref=cut(p), dst_ref=fbuf.at[slot], send_sem=a_send.at[p], recv_sem=a_recv.at[slot],
            device_id={"blk": p})

    barrier = pltpu.get_barrier_semaphore()
    for k in (4, 3, 5, 2, 6, 1, 7):
        signal(barrier, blk=at(my, mz + k, mx))
    for k in range(1, NX):
        signal(barrier, blk=at(my, mz, mx + k))
    for k in range(1, NY):
        signal(barrier, blk=at(my + k, mz, mx))
    signal(barrier, grp=other)
    pl.semaphore_wait(barrier, NZ + NX + NY - 2)
    for k in range(1, NX):
        signal(phase.at[0], blk=at(my, mz, mx + k))

    def far(i):
        return 4 + (i // 2) * (1 - i % 2) - ((i + 1) // 2) * (i % 2) + NZ

    def send_line(i, _):
        copy(at(my, mz + far(i), mx), me).start()
        return 0

    lax.fori_loop(0, NZ - 1, send_line, 0)
    local = [
        pltpu.make_async_copy(cut(me), fbuf.at[slot_of(me)], own_sem.at[0]),
        pltpu.make_async_copy(weight_in, weight_ref, own_sem.at[1]),
        pltpu.make_async_copy(response_in, response_ref, own_sem.at[2]),
        pltpu.make_async_copy(table_in, table_ref, own_sem.at[3]),
    ]
    for each in local:
        each.start()
    pl.semaphore_wait(phase.at[0], NX - 1)
    for k in range(1, NY):
        signal(phase.at[1], blk=at(my + k, mz, mx))

    def send_plane(i, _):
        copy(at(my, mz + far(i % NZ), mx + 1 + i // NZ), me).start()
        return 0

    lax.fori_loop(0, PLANE - NZ, send_plane, 0)
    pl.semaphore_wait(phase.at[1], NY - 1)

    def send_rest(i, _):
        copy(at(my + 1 + i // PLANE, mz + far(i % NZ), mx + (i // NZ) % NX), me).start()
        return 0

    lax.fori_loop(0, NB - PLANE, send_rest, 0)

    f_ref[...] = jnp.zeros_like(f_ref)
    for each in local:
        each.wait()
    gain = response_ref[...]
    filt_ref[...] = (
        dot_t(table_ref[2] * gain, table_ref[0], TOP) + dot_t(table_ref[3] * gain, table_ref[1], TOP))

    share = GROUP // 2
    owner_group = (my + 1) % NY

    def pair(t, group):
        return pltpu.make_async_remote_copy(
            src_ref=gacc.at[aligned(group * GROUP + other * share, share)], dst_ref=pbuf.at[t],
            send_sem=p_send.at[t], recv_sem=p_recv.at[t], device_id={"grp": other})

    def s1(t, i, group, slot):
        return pltpu.make_async_remote_copy(
            src_ref=hbuf.at[t, aligned(i * 8, 8)], dst_ref=s1buf.at[slot], send_sem=s1_send.at[t * NX + i],
            recv_sem=s1_recv.at[slot], device_id={"blk": at(group + NY - 1, mz, i)})

    def s1_from(p):
        return pltpu.make_async_remote_copy(
            src_ref=hbuf.at[0, aligned(0, 8)], dst_ref=s1buf.at[p], send_sem=s1_send.at[0],
            recv_sem=s1_recv.at[p], device_id={"blk": xy_peer(p)})

    def window(t):
        group = (my + NY - t) % NY

        def batch(q, _):
            x = (mx + NX - q) % NX

            def arrive(i, _):
                p = at(group, mz + i, x)
                copy(p, p).wait_recv()
                return 0

            lax.fori_loop(jnp.where(t + q == 0, 1, 0), NZ, arrive, 0)
            start = x * BLOCK

            def unpack(c, _):
                lanes = aligned(c * CHUNK, CHUNK)
                block = fbuf[aligned(group * PLANE + x * NZ, NZ), :, lanes].reshape(BLOCK, CHUNK)
                f_ref[aligned(group * GROUP + start, BLOCK), lanes] = block
                w = weight_ref[:, lanes]
                for k, part in enumerate(split3(block.astype(jnp.float32) * (w * w))):
                    pieces[aligned(k * GROUP + start, BLOCK), lanes] = part
                return 0

            lax.fori_loop(0, ROWS // CHUNK, unpack, 0)
            return 0

        lax.fori_loop(0, NX, batch, 0)
        rows = aligned(group * GROUP, GROUP)
        terms = dot_t(pieces[...], f_ref[...])
        total = terms[2 * GROUP:, :] + terms[GROUP:2 * GROUP, :] + terms[:GROUP, :]
        column = lax.broadcasted_iota(jnp.int32, (GROUP, COLS), 1)
        gacc[rows, :] = jnp.where(column // GROUP == group, 0.5 * total, total)
        pair(t, group).start()
        pair(t, group).wait_recv()
        hbuf[t] = gacc[aligned(group * GROUP + core * share, share), :] + pbuf[t]
        return group

    def early(t, _):
        group = window(t)
        for i in range(NX):
            s1(t, i, group, mxy).start()
        return 0

    lax.fori_loop(0, NY - 1, early, 0)
    window(NY - 1)
    row = [(mx + k) % NX for k in range(1, NX)]
    for i in row:
        s1(NY - 1, i, owner_group, mxy).start()

    def s2(p, slot):
        return pltpu.make_async_remote_copy(
            src_ref=tbuf.at[0], dst_ref=s2buf.at[slot], send_sem=s2_send.at[p], recv_sem=s2_recv.at[slot],
            device_id={"blk": at(my, p, mx)})

    def piece(p, c):
        y, x = p // NX, p % NX
        return aligned(((y + 1) % NY) * GROUP + c * share + x * 8, 8)

    def s3(p, c, q, d):
        return pltpu.make_async_remote_copy(
            src_ref=tbuf.at[1], dst_ref=g_ref.at[piece(q, d)],
            send_sem=s3_send.at[c * 16 + p], recv_sem=s3_recv.at[d * 16 + q], device_id={"blk": xy_peer(p), "grp": c})

    xy = [(my + y) % NY * NX + (mx + x) % NX for y, x in FAR_FIRST]
    line = [(mz + k) % NZ for k in (4, 3, 5, 2, 6, 1, 7)]
    total = hbuf[NY - 1, aligned(mx * 8, 8), :]
    for k in range(1, NY):
        for j in range(NX):
            p = (my + k) % NY * NX + j
            s1_from(p).wait_recv()
            total = total + s1buf[p]
    for i in row:
        p = my * NX + i
        s1_from(p).wait_recv()
        total = total + s1buf[p]
    tbuf[0] = total
    s2buf[mz] = total
    for p in line:
        s2(p, mz).start()

    def sent(k, _):
        copy((me + k) % NB, me).wait_send()
        return 0

    lax.fori_loop(1, NB, sent, 0)

    def shared(t, _):
        group = (my + NY - t) % NY
        pair(t, group).wait_send()
        for i in range(NX):
            s1(t, i, group, mxy).wait_send()
        return 0

    lax.fori_loop(0, NY - 1, shared, 0)
    pair(NY - 1, owner_group).wait_send()
    for i in row:
        s1(NY - 1, i, owner_group, mxy).wait_send()

    for p in line:
        s2(p, p).wait_recv()
    total = s2buf[0]
    for k in range(1, NZ):
        total = total + s2buf[k]
    tbuf[1] = total
    g_ref[piece(mxy, core), :] = total
    for p in xy:
        s3(p, core, mxy, core).start()
        s3(p, other, mxy, core).start()
    s3(mxy, other, mxy, core).start()
    for p in xy:
        s3(p, core, p, core).wait_recv()
        s3(p, other, p, other).wait_recv()
    s3(mxy, other, mxy, other).wait_recv()
    for p in xy:
        s3(p, core, mxy, core).wait_send()
        s3(p, other, mxy, core).wait_send()
    s3(mxy, other, mxy, core).wait_send()
    for p in line:
        s2(p, p).wait_send()


def gather_and_gram(field, weight, response, table):
    dma = pltpu.SemaphoreType.DMA
    vmem = pl.BlockSpec(memory_space=pltpu.VMEM)
    hbm = pl.BlockSpec(memory_space=pltpu.HBM)
    return pl.pallas_call(
        gather_kernel,
        out_shape=(
            jax.ShapeDtypeStruct((COLS, ROWS), jnp.bfloat16),
            jax.ShapeDtypeStruct((COLS, COLS), jnp.float32),
            jax.ShapeDtypeStruct((MONTHS, MONTHS), jnp.float32),
            jax.ShapeDtypeStruct((1, ROWS), jnp.float32),
        ),
        in_specs=[hbm, hbm, hbm, hbm],
        out_specs=(vmem, vmem, vmem, vmem),
        scratch_shapes=[
            pltpu.VMEM((1, BINS), jnp.float32),
            pltpu.VMEM((4, MONTHS, BINS), jnp.float32),
            pltpu.VMEM((NB, 2, ROWS), jnp.bfloat16),
            pltpu.VMEM((COLS, COLS), jnp.float32),
            pltpu.VMEM((3 * GROUP, ROWS), jnp.bfloat16),
            pltpu.VMEM((NY, GROUP // 2, COLS), jnp.float32),
            pltpu.VMEM((NY, GROUP // 2, COLS), jnp.float32),
            pltpu.VMEM((16, 8, COLS), jnp.float32),
            pltpu.VMEM((NZ, 8, COLS), jnp.float32),
            pltpu.VMEM((2, 8, COLS), jnp.float32),
            pltpu.SemaphoreType.REGULAR((2,)),
            dma((4,)), dma((NB,)), dma((NB,)), dma((NY,)), dma((NY,)),
            dma((16,)), dma((16,)), dma((NZ,)), dma((NZ,)), dma((32,)), dma((32,)),
        ],
        compiler_params=pltpu.CompilerParams(
            collective_id=0, has_side_effects=True, vmem_limit_bytes=16 * 1024 * 1024),
        name="gather_gram",
    )(field, weight, response, table)


def shards(field, response, area_weight):
    gathered, raw, filt, weight = gather_and_gram(
        *(pltpu.with_memory_space_constraint(x, pltpu.HBM) for x in (field, area_weight.reshape(1, ROWS), response.reshape(1, BINS), jnp.asarray(filter_tables()))))
    return solve(raw, filt, weight, gathered)


def solution(mesh):
    in_specs = (P("blk", "grp"), P(), P(("grp", "blk")))
    out_specs = (P(None, ("grp", "blk")), P())
    return jax.shard_map(shards, mesh=mesh, in_specs=in_specs, out_specs=out_specs, check_vma=False)
```
